32 devices in a mesh: ep: 8 (over z, x), dp: 4 (over y, core).
Axes of the slice: x: 2, y: 2, z: 4, core: 2. Of those that a mesh axis runs over, the one named last changes fastest.
Arguments:
- residual: bfloat16 [4096, 2880], P(('ep', 'dp')), may hold values from -400 to 400, as said below
- norm_gain: float32 [2880], replicated, may hold values from 0.25 to 1.75
- router_weight: bfloat16 [2880, 32], replicated, may hold values from -0.109375 to 0.109375
- out_grad: bfloat16 [4096, 2880], P(('ep', 'dp')), may hold values from -6 to 6
- expert_ids: int32 [4096, 4], P(('ep', 'dp')), may hold values from 0 to 31, all different within a row; in each aligned block of 128 rows (0 to 127, 128 to 255, ...) at most 24 rows name the same one
- hidden: bfloat16 [32, 768, 1440], P(('ep', 'dp')), may hold values from -0.3125 to 0.3125
- down_weight: bfloat16 [32, 1440, 2880], P(('ep', 'dp')), may hold values from -0.15625 to 0.15625
Outputs:
- hidden_grad: bfloat16 [32, 768, 1440], P(('ep', 'dp'))
- down_weight_grad: bfloat16 [32, 1440, 2880], P(('ep', 'dp'))
- residual_grad: bfloat16 [4096, 2880], P(('ep', 'dp'))
- router_grad: float32 [2880, 32], replicated
- gain_grad: float32 [2880], replicated
The draws below stay inside these ranges and needn't reach their ends.
Inputs may be any that keep to these rules, and one draw needn't show every extreme that they name: `expert_ids`: in the tokens of one device no expert is named more than 24 times, a bound that some block reaches. `residual`: Real-valued entries.
All inputs are finite; a program needn't handle non-finite values.
Results may differ from the reference program's by a relative error of at most 0.0085.
Values may be sent and summed in bfloat16 or wider, within the bound.
A program may use at most 128 MiB of HBM per device.

```python
import math
import jax
import jax.numpy as jnp
import numpy as np
from jax import lax

D = 2880
TOPK = 4
FF = 1440
TOK_DEV = 128
EXPERTS = 32
TOKENS = 4096
CAP = 24
SLOTS = 768
N_EP = 8
N_DP = 4


def draw_residual(key, part):
    key_rows, key_cols, key_base = jax.random.split(key, 3)
    row_scale = jnp.exp(jax.random.uniform(key_rows, (TOKENS, 1), jnp.float32, 0.0, math.log(10.0)))
    column_scale = jnp.exp(jax.random.uniform(key_cols, (1, D), jnp.float32, 0.0, math.log(10.0)))
    base = jax.random.truncated_normal(key_base, -3.5, 3.5, (TOKENS, D), jnp.float32)
    return (base * row_scale * column_scale).astype(jnp.bfloat16)


def shard_levels(own_key, dims, pieces, least, high):
    loudness = 1.0
    for dim, shards_of in pieces:
        draws = jax.random.uniform(jax.random.fold_in(jax.random.fold_in(own_key, 6), dim), (shards_of,), jnp.float32, least / len(pieces), high / len(pieces))
        loudness = loudness * jnp.repeat(jnp.exp(draws), dims[dim] // shards_of).reshape((-1,) + (1,) * (len(dims) - 1 - dim))
    return loudness


def deal_out(key, own, number, rows, number_of, top, reach, skew):
    sequence = jax.random.permutation(key, number_of)
    crowded, ordinary = load_shares(number_of, rows * top, reach, skew, True), load_shares(number_of, rows * top, reach, skew, False)
    places = jnp.arange(number_of)

    def named(tallies, turn):
        used = int((tallies > 0).sum())
        fixed = max(1, used // 4)
        passed = fixed + (places - fixed + turn * (used - fixed)) % max(1, number_of - fixed)
        return jnp.zeros((number_of,), jnp.int32).at[sequence[jnp.where(places < fixed, places, passed)]].set(jnp.asarray(tallies, jnp.int32))

    tallies = jnp.where(number % 4 == 0, named(crowded, number // 4), named(ordinary, number - number // 4 - 1))
    mixed = jax.random.permutation(jax.random.fold_in(own, 3), number_of)
    source_of, sink = mixed[0:number_of // 2 * 2:2], mixed[1:number_of // 2 * 2:2]
    slack = jnp.minimum(tallies[source_of] - 1, reach - tallies[sink]) // 2
    slack = jnp.where((source_of == sequence[0]) | (sink == sequence[0]) | (tallies[sink] == 0), 0, jnp.maximum(slack, 0))
    passed = jax.random.randint(jax.random.fold_in(own, 4), (number_of // 2,), 0, 1 << 20) % (slack + 1)
    tallies = tallies.at[source_of].add(-passed).at[sink].add(passed)
    items = jnp.searchsorted(jnp.cumsum(tallies), jnp.arange(rows * top), side="right").astype(jnp.int32)
    grid = items.reshape(top, rows).T
    grid = grid[jax.random.permutation(jax.random.fold_in(own, 1), rows)]
    turn = jax.random.randint(jax.random.fold_in(own, 2), (rows, 1), 0, top)
    return jnp.take_along_axis(grid, (jnp.arange(top)[None, :] + turn) % top, axis=1)


def load_shares(count, total, reach, slope, full):
    weights = [(1 << 20) // math.isqrt(standing ** slope) + 1 for standing in range(1, count + 1)]
    largest = reach if full else min(reach, max(-(-total // count), total * weights[0] // sum(weights)))
    least = 1 if total - largest >= count - 1 else 0
    given, rest = [largest] + [least] * (count - 1), total - largest - least * (count - 1)
    while rest > 0:
        free = [i for i in range(1, count) if given[i] < largest] or [i for i in range(1, count) if given[i] < reach]
        mass, remaining = sum([weights[i] for i in free]), rest
        for i in free:
            addition = min(reach - given[i], max(1, remaining * weights[i] // mass), rest)
            given[i] = given[i] + addition
            rest = rest - addition
    return np.array(given)


def scatter_about(rng, shape, scale, limit, shards=(), held_as=jnp.bfloat16):
    level = shard_levels(rng, shape, shards, -0.22, 0.18) if shards else 1.0
    values = jax.random.normal(rng, shape, jnp.float32) * scale * level
    return jnp.minimum(jnp.maximum(values, -limit), limit).astype(held_as)


def setup_inputs(seed: int = 0) -> dict:
    streams_of = jax.random.split(jax.random.key(seed), 8)
    residual = draw_residual(jax.random.fold_in(streams_of[7], 71), 0)
    norm_gain = jnp.clip(1.0 + 0.15 * jax.random.normal(streams_of[1], (D,), jnp.float32), 0.25, 1.75)
    router_weight = scatter_about(streams_of[2], (D, EXPERTS), D ** -0.5, 0.109375)
    out_grad = scatter_about(streams_of[3], (TOKENS, D), 1.0, 6.0, ((0, 32),))
    expert_ids_keys = jax.random.split(jax.random.fold_in(streams_of[4], 1), TOKENS // TOK_DEV)
    expert_ids_turns = jax.random.permutation(jax.random.fold_in(streams_of[4], 3), TOKENS // TOK_DEV)
    expert_ids = jax.vmap(lambda own, number: deal_out(jax.random.fold_in(streams_of[4], 2), own, number, TOK_DEV, EXPERTS, TOPK, CAP, 2))(expert_ids_keys, expert_ids_turns).reshape((TOKENS, TOPK))
    hidden = scatter_about(streams_of[5], (EXPERTS, SLOTS, FF), 0.05, 0.3125, ((0, 32),))
    down_weight = scatter_about(streams_of[6], (EXPERTS, FF, D), FF ** -0.5, 0.15625, ((0, 32),))
    return {"residual": residual, "norm_gain": norm_gain, "router_weight": router_weight, "out_grad": out_grad, "expert_ids": expert_ids, "hidden": hidden, "down_weight": down_weight}


def expert_step(packed):
    sent_grad, sent_prob, hidden_rows, weight = packed
    inner = lax.dot_general(sent_grad, weight, (((1,), (1,)), ((), ())), preferred_element_type=jnp.float32)
    slot_score = lax.optimization_barrier(jnp.sum(inner * hidden_rows.astype(jnp.float32), -1))
    weight_col = sent_prob.astype(jnp.float32)[:, None]
    hidden_grad = (weight_col * inner).astype(jnp.bfloat16)
    scaled = (weight_col * sent_grad.astype(jnp.float32)).astype(jnp.bfloat16)
    weight_grad = lax.dot_general(hidden_rows, scaled, (((0,), (0,)), ((), ())), preferred_element_type=jnp.float32)
    return (slot_score, hidden_grad, weight_grad.astype(jnp.bfloat16))

def reference(residual, norm_gain, router_weight, out_grad, expert_ids, hidden, down_weight):
    sources = N_EP * N_DP
    floated = residual.astype(jnp.float32)
    inverse = lax.rsqrt(lax.optimization_barrier(jnp.mean(floated * floated, -1, keepdims=True)) + 1e-05)
    unit = floated * inverse
    normed = (unit * norm_gain).astype(jnp.bfloat16)
    logits = jnp.dot(normed, router_weight, preferred_element_type=jnp.float32)
    picked = jnp.take_along_axis(logits, expert_ids, 1)
    expo = jnp.exp(picked)
    prob = expo / lax.optimization_barrier(jnp.sum(expo, -1, keepdims=True))
    flat_ids = expert_ids.reshape(sources, TOK_DEV * TOPK)
    onehot = (flat_ids[:, :, None] == jnp.arange(EXPERTS, dtype=jnp.int32)[None, None, :]).astype(jnp.int32)
    before = jnp.cumsum(onehot, 1) - onehot
    slot_rank = lax.optimization_barrier(jnp.sum(before * onehot, -1))
    source_idx = jnp.arange(sources, dtype=jnp.int32)[:, None]
    place = (flat_ids * SLOTS + source_idx * CAP + slot_rank).reshape(-1).astype(jnp.int32)
    repeated = jnp.repeat(out_grad, TOPK, axis=0)
    sent_grad = jnp.zeros((EXPERTS * SLOTS, D), jnp.bfloat16).at[place].set(repeated).reshape(EXPERTS, SLOTS, D)
    sent_prob = jnp.zeros((EXPERTS * SLOTS,), jnp.bfloat16).at[place].set(prob.astype(jnp.bfloat16).reshape(-1)).reshape(EXPERTS, SLOTS)
    slot_score, hidden_grad, down_weight_grad = lax.map(expert_step, (sent_grad, sent_prob, hidden, down_weight))
    score = slot_score.reshape(-1)[place].reshape(TOKENS, TOPK)
    pick_grad = prob * (score - lax.optimization_barrier(jnp.sum(prob * score, -1, keepdims=True)))
    match = expert_ids[:, :, None] == jnp.arange(EXPERTS, dtype=jnp.int32)[None, None, :]
    logit_grad = lax.optimization_barrier(jnp.sum(jnp.where(match, pick_grad[:, :, None], jnp.float32(0.0)), 1))
    router_grad = jnp.dot(normed.astype(jnp.float32).T, logit_grad, precision=lax.Precision.HIGHEST)
    normed_grad = jnp.dot(logit_grad, router_weight.astype(jnp.float32).T, precision=lax.Precision.HIGHEST)
    gain_grad = lax.optimization_barrier(jnp.sum(normed_grad * unit, 0))
    upper = normed_grad * norm_gain
    residual_grad = (inverse * (upper - unit * lax.optimization_barrier(jnp.mean(upper * unit, -1, keepdims=True)))).astype(jnp.bfloat16)
    return (hidden_grad, down_weight_grad, residual_grad, router_grad, gain_grad)
```

```python
import functools
import math

import jax
import jax.numpy as jnp
from jax import lax
from jax.experimental import pallas as pl
from jax.experimental.pallas import tpu as pltpu
from jax.sharding import PartitionSpec as P

F32 = jnp.float32
BF16 = jnp.bfloat16
LINE = 4
PIECES = 3


def kernel(
    n_ep, n_dp, lines, cap, cuts,
    res_any, gain_any, rwt_any, og_any, ids_any, hidt_any, w_any,
    hgt, wg, rg_ref, rgt_ref, gg_ref,
    res_s, gain_s, rwt_s, ids_s, tok, meta, metat, hot_s, send, recv, w, hid3, hidt, inner_s, scaled, normed_s, inv_s,
    prob_s, rank_s, ssend, srecv, part, rsbuf, agbuf,
    in_sem, tok_send, tok_recv, meta_send, meta_recv, row_send, row_recv, sc_send, sc_recv, rs_send, rs_recv, ag_send, ag_recv,
):
    n = n_ep * n_dp
    width, tokens = res_s.shape
    experts = rwt_s.shape[0]
    ff = w.shape[0]
    pad_width = send.shape[2]
    plane = n // lines
    group = plane * cap
    pieces = len(cuts)
    owned = part.shape[0]
    me = lax.axis_index("ep") * n_dp + lax.axis_index("dp")
    mine = (me * owned + n - 1) // n
    owner = mine * n < (me + 1) * owned
    z = me // plane
    p = me % plane

    def remote(src, dst, s_sem, r_sem, dev_ep, dev_dp):
        return pltpu.make_async_remote_copy(
            src_ref=src, dst_ref=dst, send_sem=s_sem, recv_sem=r_sem,
            device_id=(dev_ep, dev_dp), device_id_type=pl.DeviceIdType.MESH,
        )

    barrier = pltpu.get_barrier_semaphore()

    def hello(to):
        pl.semaphore_signal(
            barrier, inc=1, device_id=(to // n_dp, to % n_dp), device_id_type=pl.DeviceIdType.MESH
        )

    for side in range(2):
        nxt = z + 2 * side - 1

        @pl.when((nxt >= 0) & (nxt < lines))
        def _():
            hello(nxt * plane + p)

    def greet(k, _):
        hello(z * plane + (p + k) % plane)
        return 0

    lax.fori_loop(1, plane, greet, 0)

    load_og = pltpu.make_async_copy(og_any, tok.at[z], in_sem.at[0])
    loads = [
        pltpu.make_async_copy(res_any, res_s, in_sem.at[1]),
        pltpu.make_async_copy(gain_any, gain_s, in_sem.at[2]),
        pltpu.make_async_copy(rwt_any, rwt_s, in_sem.at[3]),
        pltpu.make_async_copy(ids_any, ids_s, in_sem.at[4]),
    ]
    load_h = pltpu.make_async_copy(hidt_any, hidt, in_sem.at[5])
    load_w = pltpu.make_async_copy(w_any, w, in_sem.at[6])
    load_og.start()
    for c in loads:
        c.start()
    load_h.start()
    load_w.start()

    def tok_copy(source, side, j):
        to = (z + 2 * side - 1) * plane + p
        at = pl.ds(cuts[j][0], cuts[j][1])
        return remote(
            tok.at[source, at], tok.at[source, at], tok_send.at[source, side], tok_recv.at[source, j],
            to // n_dp, to % n_dp,
        )

    def meta_copy(source, side):
        to = (z + 2 * side - 1) * plane + p
        return remote(
            meta.at[source], meta.at[source], meta_send.at[source, side], meta_recv.at[source],
            to // n_dp, to % n_dp,
        )

    def along(source, side, j):
        return [tok_copy(source, side, j)] + ([meta_copy(source, side)] if j == 0 else [])

    def to_side(side, copies):
        nxt = z + 2 * side - 1

        @pl.when((nxt >= 0) & (nxt < lines))
        def _():
            for c in copies:
                c.start()

    ssend[...] = jnp.zeros_like(ssend)
    part[owned - 1] = jnp.zeros(part.shape[1:], BF16)
    load_og.wait()
    neighbours = jnp.where(z > 0, 1, 0) + jnp.where(z < lines - 1, 1, 0)
    pl.semaphore_wait(barrier, plane - 1 + neighbours)
    for side in range(2):
        to_side(side, [tok_copy(z, side, 0)])

    for c in loads:
        c.wait()
    gain_row = gain_s[...].reshape(1, width)
    gain = jnp.broadcast_to(gain_row, (tokens, width)).T
    floated = res_s[...].astype(F32)
    inverse = lax.rsqrt(jnp.mean(floated * floated, 0, keepdims=True) + 1e-05)
    unit = floated * inverse
    normed = (unit * gain).astype(BF16)
    inv_s[...] = inverse
    normed_s[...] = normed
    logits = jnp.dot(rwt_s[...], normed, preferred_element_type=F32)
    row_e = lax.broadcasted_iota(jnp.int32, (experts, tokens), 0)
    match = jnp.zeros((experts, tokens), F32)
    ids = ids_s[...]
    for k in range(ids.shape[0]):
        match = match + jnp.where(ids[k : k + 1, :] == row_e, F32(1.0), F32(0.0))
    expo = jnp.where(match > 0, jnp.exp(logits), F32(0.0))
    prob = expo / jnp.sum(expo, 0, keepdims=True)
    row_t = lax.broadcasted_iota(jnp.int32, (tokens, tokens), 0)
    col_t = lax.broadcasted_iota(jnp.int32, (tokens, tokens), 1)
    before = jnp.where(row_t < col_t, F32(1.0), F32(0.0)).astype(BF16)
    rank = jnp.dot(match.astype(BF16), before, preferred_element_type=F32)
    rank = jnp.where(match > 0, rank, F32(-1.0))
    prob_s[...] = prob
    rank_s[...] = rank
    meta[z] = jnp.concatenate([rank, prob], 0).astype(BF16)

    for side in range(2):
        to_side(side, [meta_copy(z, side)])
    for j in range(1, pieces):
        for side in range(2):
            to_side(side, [tok_copy(z, side, j)])

    def sides(k, fn):
        def step(i, _):
            source = z + k * (2 * i - 1)

            @pl.when((source >= 0) & (source < lines) & (k + 1 - i > 0) & (k >= 0))
            def _():
                fn(source, i)
            return 0
        lax.fori_loop(0, 2, step, 0)

    def onward(i):
        nxt = z + 1 - 2 * i
        return (nxt >= 0) & (nxt < lines)

    def relay(j, source, i):
        @pl.when(onward(i))
        def _():
            for c in along(source, i, j):
                c.wait_recv()
            for c in along(source, 1 - i, j):
                c.start()

    def settle(j, source, i):
        @pl.when(jnp.logical_not(onward(i)))
        def _():
            for c in along(source, i, j):
                c.wait_recv()

    def cols(j):
        return cuts[j][0], cuts[j][1] + (pad_width - width if j == 0 else 0)

    def pack(j, source, i):
        first = source * plane
        lane0, lanes = cuts[j]
        if j == 0:
            metat[...] = meta[source].astype(F32).reshape(2 * experts, 1, tokens)
            rt = metat[pl.ds(z * plane, plane)]
            pt = metat[pl.ds(experts + z * plane, plane)]
            slot = lax.broadcasted_iota(jnp.int32, (plane, cap, tokens), 1).astype(F32)
            hit = slot == rt
            hot = jnp.where(hit, F32(1.0), F32(0.0)).reshape(group, tokens).astype(BF16)
            weight = jnp.sum(jnp.where(hit, pt, F32(0.0)), -1, keepdims=True)
            hot_s[i] = hot
            send[pl.ds(first, plane), :, pl.ds(width, pad_width - width)] = jnp.broadcast_to(
                weight, (plane, cap, pad_width - width)
            ).astype(BF16)
        else:
            hot = hot_s[i]
        rows = lax.dot_general(
            hot, tok[source, pl.ds(lane0, lanes)], (((1,), (1,)), ((), ())), preferred_element_type=F32
        )
        send[pl.ds(first, plane), :, pl.ds(lane0, lanes)] = rows.reshape(plane, cap, lanes).astype(BF16)
        own = first + p
        at = pl.ds(*cols(j))
        recv[own, :, at] = send[own, :, at]

        def push(k, _):
            row_copy(source, (p + k) % plane, p, j).start()
            return 0

        lax.fori_loop(1, plane, push, 0)

    def row_copy(source, q, slot, j):
        first = source * plane
        to = z * plane + q
        at = pl.ds(*cols(j))
        return remote(
            send.at[first + q, :, at], recv.at[first + slot, :, at], row_send.at[0], row_recv.at[source, j],
            to // n_dp, to % n_dp,
        )

    def all_of(ref, s_sem, r_sem):
        return remote(ref, ref, s_sem, r_sem, 0, 0)

    def chunk(j, source, i):
        first = source * plane
        lane0, lanes = cuts[j]

        landed = recv.at[pl.ds(first, plane - 1), :, pl.ds(*cols(j))]
        all_of(landed, row_send.at[0], row_recv.at[source, j]).wait_recv()
        at = pl.ds(pl.multiple_of(first * cap, group), group)
        tail = recv[pl.ds(first, plane), :, pl.ds(pad_width - 128, 128)].astype(F32).reshape(group, 128)
        weight = tail[:, width - pad_width + 128 : width - pad_width + 129]
        grad = recv[pl.ds(first, plane), :, pl.ds(lane0, lanes)].astype(F32).reshape(group, lanes)
        inner = lax.dot_general(
            w[:, lane0 : lane0 + lanes], grad.astype(BF16), (((1,), (1,)), ((), ())), preferred_element_type=F32
        )
        if j > 0:
            inner = inner_s[i] + inner
        if j < pieces - 1:
            inner_s[i] = inner
        else:
            score = jnp.sum(inner * hid3[source].astype(F32), 0, keepdims=True)
            for k in range(plane):
                ssend[first + k, :, pl.ds(0, cap)] = score[:, k * cap : (k + 1) * cap]

            def push(k, _):
                d = first + k

                @pl.when(d != me)
                def _():
                    remote(
                        ssend.at[d], srecv.at[me], sc_send.at[0], sc_recv.at[0], d // n_dp, d % n_dp
                    ).start()
                return 0

            lax.fori_loop(0, plane, push, 0)

            @pl.when(source == z)
            def _():
                srecv[me] = ssend[me]

            across = jnp.broadcast_to(weight, (group, 128)).T[0:1, :]
            grad_h = (across * inner).astype(BF16)
            for b in range(lines):
                @pl.when(source == b)
                def _(b=b):
                    hgt[:, b * group : (b + 1) * group] = grad_h
        scaled[at, lane0 : lane0 + lanes] = (weight * grad).astype(BF16)

    def stage(k, _):
        for j in range(pieces):
            @pl.when((k > 0) & (k < lines))
            def _(j=j):
                sides(k, functools.partial(settle, j))

            @pl.when(k < lines)
            def _(j=j):
                sides(k, functools.partial(pack, j))

            later = k + (j + 1) // pieces

            @pl.when((later > 0) & (later < lines))
            def _(j=j, later=later):
                sides(later, functools.partial(relay, (j + 1) % pieces))

            if j == min(1, pieces - 1):
                @pl.when(k == 0)
                def _():
                    load_h.wait()
                    for i in range(lines):
                        hid3[i] = hidt[:, i * group : (i + 1) * group]
                    load_w.wait()

            if j > 0:
                sides(k, functools.partial(chunk, j - 1))
            else:
                sides(k - 1, functools.partial(chunk, pieces - 1))
        return 0

    lax.fori_loop(0, lines + 1, stage, 0)

    blocks = max(b for b in range(1, 6) if ff % (b * 16) == 0)
    rows_of = ff // blocks

    def wg_block(b, _):
        at = pl.ds(pl.multiple_of(b * rows_of, rows_of), rows_of)
        wg[at] = jnp.dot(hidt[at], scaled[...], preferred_element_type=F32).astype(BF16)
        return 0

    def others(fn):
        def step(i, _):
            @pl.when(i != me)
            def _():
                fn(i)
            return 0
        lax.fori_loop(0, n, step, 0)

    cut1, cut2 = (2 * blocks) // 5, (4 * blocks) // 5
    lax.fori_loop(0, cut1, wg_block, 0)

    all_of(srecv.at[pl.ds(0, n - 1)], sc_send.at[0], sc_recv.at[0]).wait_recv()
    back = srecv[...].reshape(n, 128)
    rank = rank_s[...]
    prob = prob_s[...]
    score = jnp.zeros((experts, tokens), F32)
    for r in range(cap):
        score = score + jnp.where(rank == F32(r), back[:, r : r + 1], F32(0.0))
    lg = prob * (score - jnp.sum(prob * score, 0, keepdims=True))
    hi = lg.astype(BF16)
    lo = (lg - hi.astype(F32)).astype(BF16)
    both = lax.dot_general(
        jnp.concatenate([hi, lo], 0), normed_s[...], (((1,), (1,)), ((), ())),
        preferred_element_type=F32,
    )
    router = (both[:experts] + both[experts:]).astype(BF16)
    for b in range(owned):
        lanes = min(128, width - b * 128)
        part[b, :, pl.ds(0, lanes)] = router[:, b * 128 : b * 128 + lanes]

    def share(b, _):
        to = b * n // owned

        @pl.when(to != me)
        def _():
            remote(part.at[b], rsbuf.at[me], rs_send.at[0], rs_recv.at[0], to // n_dp, to % n_dp).start()
        return 0

    lax.fori_loop(0, owned, share, 0)

    @pl.when(owner)
    def _():
        rsbuf[me] = part[mine]

    lax.fori_loop(cut1, cut2, wg_block, 0)

    @pl.when(owner)
    def _():
        all_of(rsbuf.at[pl.ds(0, n - 1)], rs_send.at[0], rs_recv.at[0]).wait_recv()
        agbuf[mine] = jnp.sum(rsbuf[...].astype(F32), 0).astype(BF16)
        others(lambda i: remote(agbuf.at[mine], agbuf.at[mine], ag_send.at[0], ag_recv.at[0], i // n_dp, i % n_dp).start())

    rwt = rwt_s[...]
    ngrad = lax.dot_general(
        jnp.concatenate([rwt, rwt], 0), jnp.concatenate([hi, lo], 0), (((0,), (0,)), ((), ())),
        preferred_element_type=F32,
    )
    upper = ngrad * jnp.broadcast_to(gain_s[...].reshape(1, width), (tokens, width)).T
    unit = res_s[...].astype(F32) * inv_s[...]
    mean = jnp.mean(upper * unit, 0, keepdims=True)
    rg_ref[...] = (inv_s[...] * (upper - unit * mean)).astype(BF16)

    lax.fori_loop(cut2, blocks, wg_block, 0)

    all_of(send.at[pl.ds(0, lines * (plane - 1))], row_send.at[0], row_recv.at[0, 0]).wait_send()

    def finish_toks(source, _):
        def sent(side):
            nxt = z + 2 * side - 1

            @pl.when((nxt >= 0) & (nxt < lines))
            def _():
                all_of(tok.at[source], tok_send.at[source, side], tok_recv.at[source, 0]).wait_send()
                meta_copy(source, side).wait_send()

        @pl.when(source <= z)
        def _():
            sent(1)

        @pl.when(source >= z)
        def _():
            sent(0)
        return 0

    lax.fori_loop(0, lines, finish_toks, 0)
    all_of(ssend.at[pl.ds(0, n - 1)], sc_send.at[0], sc_recv.at[0]).wait_send()

    @pl.when(owner)
    def _():
        all_of(part.at[pl.ds(0, owned - 1)], rs_send.at[0], rs_recv.at[0]).wait_send()
        all_of(agbuf.at[pl.ds(0, owned - 1)], ag_send.at[0], ag_recv.at[0]).wait_recv()

    @pl.when(jnp.logical_not(owner))
    def _():
        all_of(part.at[pl.ds(0, owned)], rs_send.at[0], rs_recv.at[0]).wait_send()
        all_of(agbuf.at[pl.ds(0, owned)], ag_send.at[0], ag_recv.at[0]).wait_recv()

    gain_row = gain_s[...].reshape(1, width)
    for b in range(owned):
        lanes = min(128, width - b * 128)
        at = slice(b * 128, b * 128 + lanes)
        total = agbuf[b, :, pl.ds(0, lanes)].astype(F32)
        rgt_ref[:, at] = total
        gg_ref[:, at] = jnp.sum(total * rwt_s[:, at].astype(F32), 0, keepdims=True) / gain_row[:, at]


    @pl.when(owner)
    def _():
        all_of(rsbuf.at[pl.ds(0, n - 1)], ag_send.at[0], ag_recv.at[0]).wait_send()


def store(hgt, wg, rg, rgt, gg, hgt_any, wg_any, rg_any, rgt_any, gg_any, sem):
    ff = wg.shape[0]
    blocks = max(b for b in range(1, 7) if ff % (b * 16) == 0)
    rows = ff // blocks
    copies = [
        pltpu.make_async_copy(wg.at[pl.ds(b * rows, rows)], wg_any.at[pl.ds(b * rows, rows)], sem.at[4 + b])
        for b in range(blocks)
    ]
    copies += [
        pltpu.make_async_copy(hgt, hgt_any, sem.at[0]),
        pltpu.make_async_copy(rg, rg_any, sem.at[1]),
        pltpu.make_async_copy(rgt, rgt_any, sem.at[2]),
        pltpu.make_async_copy(gg.at[0], gg_any, sem.at[3]),
    ]
    for c in copies:
        c.start()
    for c in copies:
        c.wait()


def column_cuts(width, pad_width, count):
    tiles = pad_width // 128
    sizes = [tiles // count + (1 if i < tiles % count else 0) for i in range(count)]
    last = (tiles - sizes[0]) * 128
    cuts = [(last, width - last)]
    at = 0
    for s in sizes[1:]:
        cuts.append((at, s * 128))
        at += s * 128
    return tuple(cuts)


def on_device(n_ep, n_dp, residual, norm_gain, router_weight, out_grad, expert_ids, hidden, down_weight):
    n = n_ep * n_dp
    lines = math.gcd(n_ep, LINE)
    tokens, width = residual.shape
    topk = expert_ids.shape[1]
    experts = router_weight.shape[1]
    slots, ff = hidden.shape[1:]
    real_cap = slots // experts
    cap = -(-real_cap // 8) * 8
    pad_width = -(-(width + 1) // 128) * 128
    hidt = hidden[0].T
    if cap != real_cap:
        hidt = jnp.pad(
            hidt.reshape(ff, experts, real_cap), ((0, 0), (0, 0), (0, cap - real_cap))
        ).reshape(ff, experts * cap)
    rows = experts * cap
    plane = n // lines
    group = plane * cap
    owned = -(-width // 128)
    assert owned <= n
    cuts = column_cuts(width, pad_width, PIECES)
    vmem = pl.BlockSpec(memory_space=pltpu.VMEM)
    anyspace = pl.BlockSpec(memory_space=pl.ANY)
    dma = pltpu.SemaphoreType.DMA

    def far(x):
        return pltpu.with_memory_space_constraint(x, pltpu.HBM)

    outs = (((ff, rows), BF16), ((ff, width), BF16), ((width, tokens), BF16), ((experts, width), F32))
    held = pl.pallas_call(
        functools.partial(kernel, n_ep, n_dp, lines, cap, cuts),
        out_shape=tuple(pltpu.VMEM(s, t) for s, t in outs) + (pltpu.VMEM((1, width), F32),),
        in_specs=[anyspace] * 7,
        out_specs=(vmem,) * 5,
        scratch_shapes=[
            pltpu.VMEM((width, tokens), BF16),
            pltpu.VMEM((width,), F32),
            pltpu.VMEM((experts, width), BF16),
            pltpu.VMEM((topk, tokens), jnp.int32),
            pltpu.VMEM((lines, width, tokens), BF16),
            pltpu.VMEM((lines, 2 * experts, tokens), BF16),
            pltpu.VMEM((2 * experts, 1, tokens), F32),
            pltpu.VMEM((2, group, tokens), BF16),
            pltpu.VMEM((n, cap, pad_width), BF16),
            pltpu.VMEM((n, cap, pad_width), BF16),
            pltpu.VMEM((ff, width), BF16),
            pltpu.VMEM((lines, ff, group), BF16),
            pltpu.VMEM((ff, rows), BF16),
            pltpu.VMEM((2, ff, group), F32),
            pltpu.VMEM((rows, width), BF16),
            pltpu.VMEM((width, tokens), BF16),
            pltpu.VMEM((1, tokens), F32),
            pltpu.VMEM((experts, tokens), F32),
            pltpu.VMEM((experts, tokens), F32),
            pltpu.VMEM((n, 1, 128), F32),
            pltpu.VMEM((n, 1, 128), F32),
            pltpu.VMEM((owned, experts, 128), BF16),
            pltpu.VMEM((n, experts, 128), BF16),
            pltpu.VMEM((owned, experts, 128), BF16),
            dma((7,)),
            dma((lines, 2)), dma((lines, PIECES)), dma((lines, 2)), dma((lines,)),
            dma((1,)), dma((lines, PIECES)), dma((1,)), dma((1,)),
            dma((1,)), dma((1,)), dma((1,)), dma((1,)),
        ],
        compiler_params=pltpu.CompilerParams(
            collective_id=0, has_side_effects=True, vmem_limit_bytes=53_000_000
        ),
        name="expert_backward",
    )(*(far(x) for x in (residual.T, norm_gain, router_weight.T, out_grad.T, expert_ids.T, hidt, down_weight[0])))
    hgt, wg, rg, rgt, gg = pl.pallas_call(
        store,
        out_shape=tuple(jax.ShapeDtypeStruct(s, t) for s, t in outs) + (jax.ShapeDtypeStruct((width,), F32),),
        in_specs=[vmem] * 5,
        out_specs=(anyspace,) * 5,
        scratch_shapes=[dma((10,))],
        compiler_params=pltpu.CompilerParams(vmem_limit_bytes=2_000_000),
        name="store",
    )(*held)
    if cap != real_cap:
        hgt = hgt.reshape(ff, experts, cap)[:, :, :real_cap].reshape(ff, slots)
    return hgt.T[None], wg[None], rg.T, rgt.T, gg


def solution(mesh):
    both = ("ep", "dp")
    return jax.shard_map(
        functools.partial(on_device, mesh.shape["ep"], mesh.shape["dp"]),
        mesh=mesh,
        in_specs=(P(both, None), P(), P(), P(both, None), P(both, None), P(both, None, None), P(both, None, None)),
        out_specs=(P(both, None, None), P(both, None, None), P(both, None), P(), P()),
        check_vma=False,
    )
```

```python
import functools
import math

import jax
import jax.numpy as jnp
from jax import lax
from jax.experimental import pallas as pl
from jax.experimental.pallas import tpu as pltpu
from jax.sharding import PartitionSpec as P

F32 = jnp.float32
BF16 = jnp.bfloat16
LINE = 4
SHARES = (9, 7, 4, 3)
PIECES = len(SHARES)
LAG = 2


def kernel(
    n_ep, n_dp, lines, cap, cuts,
    res_any, gain_any, rwt_any, og_any, ids_any, hidt_any, w_any,
    hgt, wg, rg_ref, rgt_ref, gg_ref,
    res_s, gain_s, rwt_s, ids_s, tok, meta, metat, hot_s, send, recv, w, hid3, hidt, inner_s, scaled, normed_t, inv_s,
    prob_s, rank_s, ssend, srecv, part, rsbuf, agbuf,
    in_sem, tok_send, tok_recv, meta_send, meta_recv, row_send, row_recv, sc_send, sc_recv, rs_send, rs_recv, ag_send, ag_recv, twin_send, twin_recv,
):
    n = n_ep * n_dp
    width, tokens = res_s.shape
    experts = rwt_s.shape[0]
    ff = w.shape[0]
    spare = send[0].shape[2] - cuts[0][1]
    plane = n // lines
    group = plane * cap
    pieces = len(cuts)
    owned = part.shape[0]
    me = lax.axis_index("ep") * n_dp + lax.axis_index("dp")
    half = owned // 2
    core = me % 2
    seat = (me // 2 * half + n // 2 - 1) // (n // 2)
    owner = seat * (n // 2) < (me // 2 + 1) * half
    mine = core * half + seat
    z = me // plane
    p = me % plane

    def remote(src, dst, s_sem, r_sem, dev_ep, dev_dp):
        return pltpu.make_async_remote_copy(
            src_ref=src, dst_ref=dst, send_sem=s_sem, recv_sem=r_sem,
            device_id=(dev_ep, dev_dp), device_id_type=pl.DeviceIdType.MESH,
        )

    barrier = pltpu.get_barrier_semaphore()

    def hello(to):
        pl.semaphore_signal(
            barrier, inc=1, device_id=(to // n_dp, to % n_dp), device_id_type=pl.DeviceIdType.MESH
        )

    for side in range(2):
        nxt = z + 2 * side - 1

        @pl.when((nxt >= 0) & (nxt < lines))
        def _():
            hello(nxt * plane + p)

    def greet(k, _):
        hello(z * plane + (p + k) % plane)
        return 0

    lax.fori_loop(1, plane, greet, 0)

    load_og = pltpu.make_async_copy(og_any, tok.at[z], in_sem.at[0])
    loads = [
        pltpu.make_async_copy(res_any, res_s, in_sem.at[1]),
        pltpu.make_async_copy(gain_any, gain_s, in_sem.at[2]),
        pltpu.make_async_copy(rwt_any, rwt_s, in_sem.at[3]),
        pltpu.make_async_copy(ids_any, ids_s, in_sem.at[4]),
    ]
    load_h = pltpu.make_async_copy(hidt_any, hidt, in_sem.at[5])
    load_w = pltpu.make_async_copy(w_any, w, in_sem.at[6])
    load_og.start()
    for c in loads:
        c.start()
    load_h.start()
    load_w.start()

    def tok_copy(source, side, j):
        to = (z + 2 * side - 1) * plane + p
        at = pl.ds(cuts[j][0], cuts[j][1])
        return remote(
            tok.at[source, at], tok.at[source, at], tok_send.at[source, side], tok_recv.at[source, j],
            to // n_dp, to % n_dp,
        )

    def meta_copy(source, side):
        to = (z + 2 * side - 1) * plane + p
        return remote(
            meta.at[source], meta.at[source], meta_send.at[source, side], meta_recv.at[source],
            to // n_dp, to % n_dp,
        )

    def along(source, side, j):
        return [tok_copy(source, side, j)] + ([meta_copy(source, side)] if j == 0 else [])

    def to_side(side, copies):
        nxt = z + 2 * side - 1

        @pl.when((nxt >= 0) & (nxt < lines))
        def _():
            for c in copies:
                c.start()

    ssend[...] = jnp.zeros_like(ssend)
    for b in range(width // 128, owned):
        part[b] = jnp.zeros(part.shape[1:], BF16)
    load_og.wait()
    neighbours = jnp.where(z > 0, 1, 0) + jnp.where(z < lines - 1, 1, 0)
    pl.semaphore_wait(barrier, plane - 1 + neighbours)
    for side in range(2):
        to_side(side, [tok_copy(z, side, 0)])

    for c in loads:
        c.wait()
    gain_row = gain_s[...].reshape(1, width)
    gain = jnp.broadcast_to(gain_row, (tokens, width)).T
    floated = res_s[...].astype(F32)
    inverse = lax.rsqrt(jnp.mean(floated * floated, 0, keepdims=True) + 1e-05)
    unit = floated * inverse
    normed = (unit * gain).astype(BF16)
    inv_s[...] = inverse
    normed_t[...] = normed.T
    logits = jnp.dot(rwt_s[...], normed, preferred_element_type=F32)
    row_e = lax.broadcasted_iota(jnp.int32, (experts, tokens), 0)
    match = jnp.zeros((experts, tokens), F32)
    ids = ids_s[...]
    for k in range(ids.shape[0]):
        match = match + jnp.where(ids[k : k + 1, :] == row_e, F32(1.0), F32(0.0))
    expo = jnp.where(match > 0, jnp.exp(logits), F32(0.0))
    prob = expo / jnp.sum(expo, 0, keepdims=True)
    row_t = lax.broadcasted_iota(jnp.int32, (tokens, tokens), 0)
    col_t = lax.broadcasted_iota(jnp.int32, (tokens, tokens), 1)
    before = jnp.where(row_t < col_t, F32(1.0), F32(0.0)).astype(BF16)
    rank = jnp.dot(match.astype(BF16), before, preferred_element_type=F32)
    rank = jnp.where(match > 0, rank, F32(-1.0))
    prob_s[...] = prob
    rank_s[...] = rank
    meta[z] = jnp.concatenate([rank, prob], 0).astype(BF16)

    for side in range(2):
        to_side(side, [meta_copy(z, side)])
    for j in range(1, pieces):
        for side in range(2):
            to_side(side, [tok_copy(z, side, j)])

    def sides(k, fn):
        def step(i, _):
            source = z + k * (2 * i - 1)

            @pl.when((source >= 0) & (source < lines) & (k + 1 - i > 0) & (k >= 0))
            def _():
                fn(source, i)
            return 0
        lax.fori_loop(0, 2, step, 0)

    def onward(i):
        nxt = z + 1 - 2 * i
        return (nxt >= 0) & (nxt < lines)

    def relay(j, source, i):
        @pl.when(onward(i))
        def _():
            for c in along(source, i, j):
                c.wait_recv()
            for c in along(source, 1 - i, j):
                c.start()

    def settle(j, source, i):
        @pl.when(jnp.logical_not(onward(i)))
        def _():
            for c in along(source, i, j):
                c.wait_recv()

    def pack(j, source, i):
        first = source * plane
        lane0, lanes = cuts[j]
        if j == 0:
            metat[...] = meta[source].astype(F32).reshape(2 * experts, 1, tokens)
            rt = metat[pl.ds(z * plane, plane)]
            pt = metat[pl.ds(experts + z * plane, plane)]
            slot = lax.broadcasted_iota(jnp.int32, (plane, cap, tokens), 1).astype(F32)
            hit = slot == rt
            hot = jnp.where(hit, F32(1.0), F32(0.0)).reshape(group, tokens).astype(BF16)
            weight = jnp.sum(jnp.where(hit, pt, F32(0.0)), -1, keepdims=True)
            hot_s[i] = hot
            send[0][pl.ds(first, plane), :, pl.ds(lanes, spare)] = jnp.broadcast_to(
                weight, (plane, cap, spare)
            ).astype(BF16)
        else:
            hot = hot_s[i]
        rows = lax.dot_general(
            hot, tok[source, pl.ds(lane0, lanes)], (((1,), (1,)), ((), ())), preferred_element_type=F32
        )
        send[j][pl.ds(first, plane), :, pl.ds(0, lanes)] = rows.reshape(plane, cap, lanes).astype(BF16)
        own = first + p
        recv[j][own] = send[j][own]

        def push(k, _):
            row_copy(source, partner(plane - k), p, j).start()
            return 0

        lax.fori_loop(1, plane, push, 0)

    def partner(k):
        if plane & (plane - 1):
            return (p + k) % plane
        bits = range(plane.bit_length() - 1)
        return sum((p // (1 << b) + k // (1 << b)) % 2 * (1 << b) for b in bits)

    def row_copy(source, q, slot, j):
        first = source * plane
        to = z * plane + q
        return remote(
            send[j].at[first + q], recv[j].at[first + slot], row_send.at[j], row_recv.at[source, j],
            to // n_dp, to % n_dp,
        )

    def all_of(ref, s_sem, r_sem):
        return remote(ref, ref, s_sem, r_sem, 0, 0)

    def chunk(j, source, i):
        first = source * plane
        lane0, lanes = cuts[j]

        landed = recv[j].at[pl.ds(first, plane - 1)]
        all_of(landed, row_send.at[j], row_recv.at[source, j]).wait_recv()
        at = pl.ds(pl.multiple_of(first * cap, group), group)
        tail = recv[0][pl.ds(first, plane), :, pl.ds(cuts[0][1] + spare - 128, 128)].astype(F32).reshape(group, 128)
        weight = tail[:, 128 - spare : 129 - spare]
        grad = recv[j][pl.ds(first, plane), :, pl.ds(0, lanes)].astype(F32).reshape(group, lanes)
        inner = lax.dot_general(
            w[:, lane0 : lane0 + lanes], grad.astype(BF16), (((1,), (1,)), ((), ())), preferred_element_type=F32
        )
        if j > 0:
            inner = inner_s[i] + inner
        if j < pieces - 1:
            inner_s[i] = inner
        else:
            score = jnp.sum(inner * hid3[source].astype(F32), 0, keepdims=True)
            for k in range(plane):
                ssend[first + k, :, pl.ds(0, cap)] = score[:, k * cap : (k + 1) * cap]

            def push(k, _):
                d = first + k

                @pl.when(d != me)
                def _():
                    remote(
                        ssend.at[d], srecv.at[me], sc_send.at[0], sc_recv.at[0], d // n_dp, d % n_dp
                    ).start()
                return 0

            lax.fori_loop(0, plane, push, 0)

            @pl.when(source == z)
            def _():
                srecv[me] = ssend[me]

            across = jnp.broadcast_to(weight, (group, 128)).T[0:1, :]
            grad_h = (across * inner).astype(BF16)
            for b in range(lines):
                @pl.when(source == b)
                def _(b=b):
                    hgt[:, b * group : (b + 1) * group] = grad_h
        scaled[at, lane0 : lane0 + lanes] = (weight * grad).astype(BF16)

    def stage(k, _):
        for j in range(pieces):
            @pl.when((k > 0) & (k < lines))
            def _(j=j):
                sides(k, functools.partial(settle, j))

            @pl.when(k < lines)
            def _(j=j):
                sides(k, functools.partial(pack, j))

            later = k + (j + 1) // pieces

            @pl.when((later > 0) & (later < lines))
            def _(j=j, later=later):
                sides(later, functools.partial(relay, (j + 1) % pieces))

            if j == min(LAG, pieces - 1):
                @pl.when(k == 0)
                def _():
                    load_h.wait()
                    for i in range(lines):
                        hid3[i] = hidt[:, i * group : (i + 1) * group]
                    load_w.wait()

            sides(k + (j - LAG) // pieces, functools.partial(chunk, (j - LAG) % pieces))
        return 0

    lax.fori_loop(0, lines + 1, stage, 0)

    blocks = max(b for b in range(1, 6) if ff % (b * 16) == 0)
    rows_of = ff // blocks

    def wg_block(b, _):
        at = pl.ds(pl.multiple_of(b * rows_of, rows_of), rows_of)
        wg[at] = jnp.dot(hidt[at], scaled[...], preferred_element_type=F32).astype(BF16)
        return 0

    cut1, cut2 = (2 * blocks) // 5, (4 * blocks) // 5
    lax.fori_loop(0, cut1, wg_block, 0)

    all_of(srecv.at[pl.ds(0, n - 1)], sc_send.at[0], sc_recv.at[0]).wait_recv()
    back = srecv[...].reshape(n, 128)
    rank = rank_s[...]
    prob = prob_s[...]
    score = jnp.zeros((experts, tokens), F32)
    for r in range(cap):
        score = score + jnp.where(rank == F32(r), back[:, r : r + 1], F32(0.0))
    lg = prob * (score - jnp.sum(prob * score, 0, keepdims=True))
    hi = lg.astype(BF16)
    lo = (lg - hi.astype(F32)).astype(BF16)
    both = jnp.dot(jnp.concatenate([hi, lo], 0), normed_t[...], preferred_element_type=F32)
    router = (both[:experts] + both[experts:]).astype(BF16)
    for b in range(-(-width // 128)):
        lanes = min(128, width - b * 128)
        part[b, :, pl.ds(0, lanes)] = router[:, b * 128 : b * 128 + lanes]

    def scatter(order):
        for at in order:
            to = at // 2 * (n // 2) // half * 2 + at % 2
            b = at % 2 * half + at // 2

            @pl.when(to != me)
            def _(to=to, b=b):
                remote(part.at[b], rsbuf.at[me], rs_send.at[0], rs_recv.at[0], to // n_dp, to % n_dp).start()

    @pl.when(z < lines // 2)
    def _():
        scatter(range(owned - 1, -1, -1))

    @pl.when(z >= lines // 2)
    def _():
        scatter(range(owned))

    @pl.when(owner)
    def _():
        rsbuf[me] = part[mine]

    lax.fori_loop(cut1, cut2, wg_block, 0)

    @pl.when(owner)
    def _():
        all_of(rsbuf.at[pl.ds(0, n - 1)], rs_send.at[0], rs_recv.at[0]).wait_recv()
        agbuf[mine] = jnp.sum(rsbuf[...].astype(F32), 0).astype(BF16)

        def spread(k, _):
            i = jnp.where(z < lines // 2, n // 2 - 1 - k, k) * 2 + core

            @pl.when(i != me)
            def _():
                remote(
                    agbuf.at[mine], agbuf.at[mine], ag_send.at[0], ag_recv.at[0], i // n_dp, i % n_dp
                ).start()
            return 0

        lax.fori_loop(0, n // 2, spread, 0)

    rwt = rwt_s[...]
    ngrad = lax.dot_general(
        jnp.concatenate([rwt, rwt], 0), jnp.concatenate([hi, lo], 0), (((0,), (0,)), ((), ())),
        preferred_element_type=F32,
    )
    upper = ngrad * jnp.broadcast_to(gain_s[...].reshape(1, width), (tokens, width)).T
    unit = res_s[...].astype(F32) * inv_s[...]
    mean = jnp.mean(upper * unit, 0, keepdims=True)
    rg_ref[...] = (inv_s[...] * (upper - unit * mean)).astype(BF16)

    lax.fori_loop(cut2, blocks, wg_block, 0)

    for j in range(pieces):
        all_of(send[j].at[pl.ds(0, lines * (plane - 1))], row_send.at[j], row_recv.at[0, j]).wait_send()

    def finish_toks(source, _):
        def sent(side):
            nxt = z + 2 * side - 1

            @pl.when((nxt >= 0) & (nxt < lines))
            def _():
                all_of(tok.at[source], tok_send.at[source, side], tok_recv.at[source, 0]).wait_send()
                meta_copy(source, side).wait_send()

        @pl.when(source <= z)
        def _():
            sent(1)

        @pl.when(source >= z)
        def _():
            sent(0)
        return 0

    lax.fori_loop(0, lines, finish_toks, 0)
    all_of(ssend.at[pl.ds(0, n - 1)], sc_send.at[0], sc_recv.at[0]).wait_send()

    @pl.when(owner)
    def _():
        all_of(part.at[pl.ds(0, owned - 1)], rs_send.at[0], rs_recv.at[0]).wait_send()
        all_of(agbuf.at[pl.ds(0, half - 1)], ag_send.at[0], ag_recv.at[0]).wait_recv()

    @pl.when(jnp.logical_not(owner))
    def _():
        all_of(part, rs_send.at[0], rs_recv.at[0]).wait_send()
        all_of(agbuf.at[pl.ds(0, half)], ag_send.at[0], ag_recv.at[0]).wait_recv()

    to = me + 1 - 2 * core
    ours = agbuf.at[pl.ds(core * half, half)]
    twin = remote(ours, ours, twin_send.at[0], twin_recv.at[0], to // n_dp, to % n_dp)
    twin.start()
    twin.wait_recv()

    gain_row = gain_s[...].reshape(1, width)
    for b in range(-(-width // 128)):
        lanes = min(128, width - b * 128)
        at = slice(b * 128, b * 128 + lanes)
        total = agbuf[b, :, pl.ds(0, lanes)].astype(F32)
        rgt_ref[:, at] = total
        gg_ref[:, at] = jnp.sum(total * rwt_s[:, at].astype(F32), 0, keepdims=True) / gain_row[:, at]


    @pl.when(owner)
    def _():
        all_of(rsbuf.at[pl.ds(0, n // 2 - 1)], ag_send.at[0], ag_recv.at[0]).wait_send()

    twin.wait_send()


def store(hgt, wg, rg, rgt, gg, hgt_any, wg_any, rg_any, rgt_any, gg_any, sem):
    ff = wg.shape[0]
    blocks = max(b for b in range(1, 7) if ff % (b * 16) == 0)
    rows = ff // blocks
    copies = [
        pltpu.make_async_copy(wg.at[pl.ds(b * rows, rows)], wg_any.at[pl.ds(b * rows, rows)], sem.at[4 + b])
        for b in range(blocks)
    ]
    copies += [
        pltpu.make_async_copy(hgt, hgt_any, sem.at[0]),
        pltpu.make_async_copy(rg, rg_any, sem.at[1]),
        pltpu.make_async_copy(rgt, rgt_any, sem.at[2]),
        pltpu.make_async_copy(gg.at[0], gg_any, sem.at[3]),
    ]
    for c in copies:
        c.start()
    for c in copies:
        c.wait()


def column_cuts(width, pad_width):
    tiles = pad_width // 128
    ends = [tiles * sum(SHARES[: i + 1]) // sum(SHARES) for i in range(PIECES)]
    sizes = [e - b for b, e in zip([0] + ends, ends)]
    last = (tiles - sizes[0]) * 128
    cuts = [(last, width - last)]
    at = 0
    for s in sizes[1:]:
        cuts.append((at, s * 128))
        at += s * 128
    return tuple(cuts)


def on_device(n_ep, n_dp, residual, norm_gain, router_weight, out_grad, expert_ids, hidden, down_weight):
    n = n_ep * n_dp
    lines = math.gcd(n_ep, LINE)
    tokens, width = residual.shape
    topk = expert_ids.shape[1]
    experts = router_weight.shape[1]
    slots, ff = hidden.shape[1:]
    real_cap = slots // experts
    cap = -(-real_cap // 8) * 8
    pad_width = -(-(width + 1) // 128) * 128
    hidt = hidden[0].T
    if cap != real_cap:
        hidt = jnp.pad(
            hidt.reshape(ff, experts, real_cap), ((0, 0), (0, 0), (0, cap - real_cap))
        ).reshape(ff, experts * cap)
    rows = experts * cap
    plane = n // lines
    group = plane * cap
    owned = -(-width // 256) * 2
    assert owned <= n
    cuts = column_cuts(width, pad_width)
    rows_of_piece = [
        pltpu.VMEM((n, cap, lanes + (pad_width - width if j == 0 else 0)), BF16) for j, (_, lanes) in enumerate(cuts)
    ]
    vmem = pl.BlockSpec(memory_space=pltpu.VMEM)
    anyspace = pl.BlockSpec(memory_space=pl.ANY)
    dma = pltpu.SemaphoreType.DMA

    def far(x):
        return pltpu.with_memory_space_constraint(x, pltpu.HBM)

    outs = (((ff, rows), BF16), ((ff, width), BF16), ((width, tokens), BF16), ((experts, width), F32))
    held = pl.pallas_call(
        functools.partial(kernel, n_ep, n_dp, lines, cap, cuts),
        out_shape=tuple(pltpu.VMEM(s, t) for s, t in outs) + (pltpu.VMEM((1, width), F32),),
        in_specs=[anyspace] * 7,
        out_specs=(vmem,) * 5,
        scratch_shapes=[
            pltpu.VMEM((width, tokens), BF16),
            pltpu.VMEM((width,), F32),
            pltpu.VMEM((experts, width), BF16),
            pltpu.VMEM((topk, tokens), jnp.int32),
            pltpu.VMEM((lines, width, tokens), BF16),
            pltpu.VMEM((lines, 2 * experts, tokens), BF16),
            pltpu.VMEM((2 * experts, 1, tokens), F32),
            pltpu.VMEM((2, group, tokens), BF16),
            rows_of_piece,
            rows_of_piece,
            pltpu.VMEM((ff, width), BF16),
            pltpu.VMEM((lines, ff, group), BF16),
            pltpu.VMEM((ff, rows), BF16),
            pltpu.VMEM((2, ff, group), F32),
            pltpu.VMEM((rows, width), BF16),
            pltpu.VMEM((tokens, width), BF16),
            pltpu.VMEM((1, tokens), F32),
            pltpu.VMEM((experts, tokens), F32),
            pltpu.VMEM((experts, tokens), F32),
            pltpu.VMEM((n, 1, 128), F32),
            pltpu.VMEM((n, 1, 128), F32),
            pltpu.VMEM((owned, experts, 128), BF16),
            pltpu.VMEM((n, experts, 128), BF16),
            pltpu.VMEM((owned, experts, 128), BF16),
            dma((7,)),
            dma((lines, 2)), dma((lines, PIECES)), dma((lines, 2)), dma((lines,)),
            dma((PIECES,)), dma((lines, PIECES)), dma((1,)), dma((1,)),
            dma((1,)), dma((1,)), dma((1,)), dma((1,)), dma((1,)), dma((1,)),
        ],
        compiler_params=pltpu.CompilerParams(
            collective_id=0, has_side_effects=True, vmem_limit_bytes=53_000_000
        ),
        name="expert_backward",
    )(*(far(x) for x in (residual.T, norm_gain, router_weight.T, out_grad.T, expert_ids.T, hidt, down_weight[0])))
    hgt, wg, rg, rgt, gg = pl.pallas_call(
        store,
        out_shape=tuple(jax.ShapeDtypeStruct(s, t) for s, t in outs) + (jax.ShapeDtypeStruct((width,), F32),),
        in_specs=[vmem] * 5,
        out_specs=(anyspace,) * 5,
        scratch_shapes=[dma((10,))],
        compiler_params=pltpu.CompilerParams(vmem_limit_bytes=2_000_000),
        name="store",
    )(*held)
    if cap != real_cap:
        hgt = hgt.reshape(ff, experts, cap)[:, :, :real_cap].reshape(ff, slots)
    return hgt.T[None], wg[None], rg.T, rgt.T, gg


def solution(mesh):
    both = ("ep", "dp")
    return jax.shard_map(
        functools.partial(on_device, mesh.shape["ep"], mesh.shape["dp"]),
        mesh=mesh,
        in_specs=(P(both, None), P(), P(), P(both, None), P(both, None), P(both, None, None), P(both, None, None)),
        out_specs=(P(both, None, None), P(both, None, None), P(both, None), P(), P()),
        check_vma=False,
    )
```

```python
import functools
import math

import jax
import jax.numpy as jnp
from jax import lax
from jax.experimental import pallas as pl
from jax.experimental.pallas import tpu as pltpu
from jax.sharding import PartitionSpec as P

F32 = jnp.float32
BF16 = jnp.bfloat16
LINE = 4
SHARES = (9, 7, 4, 3)
PIECES = len(SHARES)
LAG = 2


def kernel(
    n_ep, n_dp, lines, cap, cuts,
    res_any, gain_any, rwt_any, og_any, ids_any, hidt_any, w_any,
    hgt, wg, rg_ref, rgt_ref, gg_ref,
    res_s, gain_s, rwt_s, ids_s, tok, meta, hot_s, send, recv, w, hid3, hidt, inner_s, scaled, normed_t, inv_s,
    prob_s, rank_s, ssend, srecv, part, rsbuf, agbuf,
    in_sem, tok_send, tok_recv, meta_send, meta_recv, row_send, row_recv, sc_send, sc_recv, rs_send, rs_recv, ag_send, ag_recv, twin_send, twin_recv,
):
    n = n_ep * n_dp
    width, tokens = res_s.shape
    experts = rwt_s.shape[0]
    ff = w.shape[0]
    spare = send[0].shape[2] - cuts[0][1]
    plane = n // lines
    group = plane * cap
    pieces = len(cuts)
    owned = part.shape[0]
    me = lax.axis_index("ep") * n_dp + lax.axis_index("dp")
    half = owned // 2
    core = me % 2
    seat = (me // 2 * half + n // 2 - 1) // (n // 2)
    owner = seat * (n // 2) < (me // 2 + 1) * half
    mine = core * half + seat
    z = me // plane
    p = me % plane

    def remote(src, dst, s_sem, r_sem, dev_ep, dev_dp):
        return pltpu.make_async_remote_copy(
            src_ref=src, dst_ref=dst, send_sem=s_sem, recv_sem=r_sem,
            device_id=(dev_ep, dev_dp), device_id_type=pl.DeviceIdType.MESH,
        )

    barrier = pltpu.get_barrier_semaphore()

    def hello(to):
        pl.semaphore_signal(
            barrier, inc=1, device_id=(to // n_dp, to % n_dp), device_id_type=pl.DeviceIdType.MESH
        )

    for side in range(2):
        nxt = z + 2 * side - 1

        @pl.when((nxt >= 0) & (nxt < lines))
        def _():
            hello(nxt * plane + p)

    def greet(k, _):
        hello(z * plane + (p + k) % plane)
        return 0

    lax.fori_loop(1, plane, greet, 0)

    load_og = pltpu.make_async_copy(og_any, tok.at[z], in_sem.at[0])
    loads = [
        pltpu.make_async_copy(res_any, res_s, in_sem.at[1]),
        pltpu.make_async_copy(gain_any, gain_s, in_sem.at[2]),
        pltpu.make_async_copy(rwt_any, rwt_s, in_sem.at[3]),
        pltpu.make_async_copy(ids_any, ids_s, in_sem.at[4]),
    ]
    load_h = pltpu.make_async_copy(hidt_any, hidt, in_sem.at[5])
    load_w = pltpu.make_async_copy(w_any, w, in_sem.at[6])
    load_og.start()
    for c in loads:
        c.start()
    load_h.start()
    load_w.start()

    def tok_copy(source, side, j):
        to = (z + 2 * side - 1) * plane + p
        at = pl.ds(cuts[j][0], cuts[j][1])
        return remote(
            tok.at[source, at], tok.at[source, at], tok_send.at[source, side], tok_recv.at[source, j],
            to // n_dp, to % n_dp,
        )

    def meta_copy(source, side):
        to = (z + 2 * side - 1) * plane + p
        return remote(
            meta.at[source], meta.at[source], meta_send.at[source, side], meta_recv.at[source],
            to // n_dp, to % n_dp,
        )

    def along(source, side, j):
        return [tok_copy(source, side, j)] + ([meta_copy(source, side)] if j == 0 else [])

    def to_side(side, copies):
        nxt = z + 2 * side - 1

        @pl.when((nxt >= 0) & (nxt < lines))
        def _():
            for c in copies:
                c.start()

    ssend[...] = jnp.zeros_like(ssend)
    for b in range(width // 128, owned):
        part[b] = jnp.zeros(part.shape[1:], BF16)
    load_og.wait()
    neighbours = jnp.where(z > 0, 1, 0) + jnp.where(z < lines - 1, 1, 0)
    pl.semaphore_wait(barrier, plane - 1 + neighbours)
    for side in range(2):
        to_side(side, [tok_copy(z, side, 0)])

    for c in loads:
        c.wait()
    gain_row = gain_s[...].reshape(1, width)
    gain = jnp.broadcast_to(gain_row, (tokens, width)).T
    floated = res_s[...].astype(F32)
    inverse = lax.rsqrt(jnp.mean(floated * floated, 0, keepdims=True) + 1e-05)
    unit = floated * inverse
    normed = (unit * gain).astype(BF16)
    inv_s[...] = inverse
    normed_t[...] = normed.T
    logits = jnp.dot(rwt_s[...], normed, preferred_element_type=F32)
    row_e = lax.broadcasted_iota(jnp.int32, (experts, tokens), 0)
    match = jnp.zeros((experts, tokens), F32)
    ids = ids_s[...]
    for k in range(ids.shape[0]):
        match = match + jnp.where(ids[k : k + 1, :] == row_e, F32(1.0), F32(0.0))
    expo = jnp.where(match > 0, jnp.exp(logits), F32(0.0))
    prob = expo / jnp.sum(expo, 0, keepdims=True)
    row_t = lax.broadcasted_iota(jnp.int32, (tokens, tokens), 0)
    col_t = lax.broadcasted_iota(jnp.int32, (tokens, tokens), 1)
    before = jnp.where(row_t < col_t, F32(1.0), F32(0.0)).astype(BF16)
    rank = jnp.dot(match.astype(BF16), before, preferred_element_type=F32)
    rank = jnp.where(match > 0, rank, F32(-1.0))
    prob_s[...] = prob
    rank_s[...] = rank
    topk = ids.shape[0]

    def chosen(values):
        return [
            jnp.sum(jnp.where(ids[k : k + 1, :] == row_e, values, F32(0.0)), 0, keepdims=True) for k in range(topk)
        ]

    unused = meta.shape[1] - 3 * topk
    info = [ids.astype(F32)] + chosen(rank) + chosen(prob)
    if unused:
        info.append(jnp.zeros((unused, tokens), F32))
    meta[z] = jnp.concatenate(info, 0).astype(BF16)

    for side in range(2):
        to_side(side, [meta_copy(z, side)])
    for j in range(1, pieces):
        for side in range(2):
            to_side(side, [tok_copy(z, side, j)])

    def sides(k, fn):
        def step(i, _):
            source = z + k * (2 * i - 1)

            @pl.when((source >= 0) & (source < lines) & (k + 1 - i > 0) & (k >= 0))
            def _():
                fn(source, i)
            return 0
        lax.fori_loop(0, 2, step, 0)

    def onward(i):
        nxt = z + 1 - 2 * i
        return (nxt >= 0) & (nxt < lines)

    def relay(j, source, i):
        @pl.when(onward(i))
        def _():
            for c in along(source, i, j):
                c.wait_recv()
            for c in along(source, 1 - i, j):
                c.start()

    def settle(j, source, i):
        @pl.when(jnp.logical_not(onward(i)))
        def _():
            for c in along(source, i, j):
                c.wait_recv()

    def pack(j, source, i):
        first = source * plane
        lane0, lanes = cuts[j]
        if j == 0:
            info = meta[source].astype(F32)
            expert = (lax.broadcasted_iota(jnp.int32, (plane, 1, tokens), 0) + z * plane).astype(F32)
            rt = jnp.full((plane, 1, tokens), -1.0, F32)
            pt = jnp.zeros((plane, 1, tokens), F32)
            for k in range(topk):
                here = expert == info[k : k + 1].reshape(1, 1, tokens)
                rt = jnp.where(here, info[topk + k : topk + k + 1].reshape(1, 1, tokens), rt)
                pt = jnp.where(here, info[2 * topk + k : 2 * topk + k + 1].reshape(1, 1, tokens), pt)
            slot = lax.broadcasted_iota(jnp.int32, (plane, cap, tokens), 1).astype(F32)
            hit = slot == rt
            hot = jnp.where(hit, F32(1.0), F32(0.0)).reshape(group, tokens).astype(BF16)
            weight = jnp.sum(jnp.where(hit, pt, F32(0.0)), -1, keepdims=True)
            hot_s[i] = hot
            send[0][pl.ds(first, plane), :, pl.ds(lanes, spare)] = jnp.broadcast_to(
                weight, (plane, cap, spare)
            ).astype(BF16)
        else:
            hot = hot_s[i]
        rows = lax.dot_general(
            hot, tok[source, pl.ds(lane0, lanes)], (((1,), (1,)), ((), ())), preferred_element_type=F32
        )
        send[j][pl.ds(first, plane), :, pl.ds(0, lanes)] = rows.reshape(plane, cap, lanes).astype(BF16)
        own = first + p
        recv[j][own] = send[j][own]

        if plane > 8:
            def push(k, _):
                row_copy(source, partner(plane - k), p, j).start()
                return 0

            lax.fori_loop(1, plane, push, 0)
        else:
            for k in range(1, plane):
                row_copy(source, partner(plane - k), p, j).start()

    def partner(k):
        if plane & (plane - 1):
            return (p + k) % plane
        bits = range(plane.bit_length() - 1)
        return sum((p // (1 << b) + k // (1 << b)) % 2 * (1 << b) for b in bits)

    def row_copy(source, q, slot, j):
        first = source * plane
        to = z * plane + q
        return remote(
            send[j].at[first + q], recv[j].at[first + slot], row_send.at[j], row_recv.at[source, j],
            to // n_dp, to % n_dp,
        )

    def all_of(ref, s_sem, r_sem):
        return remote(ref, ref, s_sem, r_sem, 0, 0)

    def chunk(j, source, i):
        first = source * plane
        lane0, lanes = cuts[j]

        landed = recv[j].at[pl.ds(first, plane - 1)]
        all_of(landed, row_send.at[j], row_recv.at[source, j]).wait_recv()
        at = pl.ds(pl.multiple_of(first * cap, group), group)
        tail = recv[0][pl.ds(first, plane), :, pl.ds(cuts[0][1] + spare - 128, 128)].astype(F32).reshape(group, 128)
        weight = tail[:, 128 - spare : 129 - spare]
        grad = recv[j][pl.ds(first, plane), :, pl.ds(0, lanes)].astype(F32).reshape(group, lanes)
        inner = lax.dot_general(
            w[:, lane0 : lane0 + lanes], grad.astype(BF16), (((1,), (1,)), ((), ())), preferred_element_type=F32
        )
        if j > 0:
            inner = inner_s[i] + inner
        if j < pieces - 1:
            inner_s[i] = inner
        else:
            score = jnp.sum(inner * hid3[source].astype(F32), 0, keepdims=True)
            for k in range(plane):
                ssend[first + k, :, pl.ds(0, cap)] = score[:, k * cap : (k + 1) * cap]

            def push(k, _):
                d = first + k

                @pl.when(d != me)
                def _():
                    remote(
                        ssend.at[d], srecv.at[me], sc_send.at[0], sc_recv.at[0], d // n_dp, d % n_dp
                    ).start()
                return 0

            lax.fori_loop(0, plane, push, 0)

            @pl.when(source == z)
            def _():
                srecv[me] = ssend[me]

            across = jnp.broadcast_to(weight, (group, 128)).T[0:1, :]
            grad_h = (across * inner).astype(BF16)
            for b in range(lines):
                @pl.when(source == b)
                def _(b=b):
                    hgt[:, b * group : (b + 1) * group] = grad_h
        scaled[at, lane0 : lane0 + lanes] = (weight * grad).astype(BF16)

    def stage(k, _):
        for j in range(pieces):
            @pl.when((k > 0) & (k < lines))
            def _(j=j):
                sides(k, functools.partial(settle, j))

            @pl.when(k < lines)
            def _(j=j):
                sides(k, functools.partial(pack, j))

            later = k + (j + 1) // pieces

            @pl.when((later > 0) & (later < lines))
            def _(j=j, later=later):
                sides(later, functools.partial(relay, (j + 1) % pieces))

            if j == min(LAG, pieces - 1):
                @pl.when(k == 0)
                def _():
                    load_h.wait()
                    for i in range(lines):
                        hid3[i] = hidt[:, i * group : (i + 1) * group]
                    load_w.wait()

            sides(k + (j - LAG) // pieces, functools.partial(chunk, (j - LAG) % pieces))
        return 0

    lax.fori_loop(0, lines + 1, stage, 0)

    blocks = max(b for b in range(1, 6) if ff % (b * 16) == 0)
    rows_of = ff // blocks

    def wg_block(b, _):
        at = pl.ds(pl.multiple_of(b * rows_of, rows_of), rows_of)
        wg[at] = jnp.dot(hidt[at], scaled[...], preferred_element_type=F32).astype(BF16)
        return 0

    cut1, cut2 = (2 * blocks) // 5, (4 * blocks) // 5
    lax.fori_loop(0, cut1, wg_block, 0)

    all_of(srecv.at[pl.ds(0, n - 1)], sc_send.at[0], sc_recv.at[0]).wait_recv()
    back = srecv[...].reshape(n, 128)
    rank = rank_s[...]
    prob = prob_s[...]
    score = jnp.zeros((experts, tokens), F32)
    for r in range(cap):
        score = score + jnp.where(rank == F32(r), back[:, r : r + 1], F32(0.0))
    lg = prob * (score - jnp.sum(prob * score, 0, keepdims=True))
    hi = lg.astype(BF16)
    lo = (lg - hi.astype(F32)).astype(BF16)
    both = jnp.dot(jnp.concatenate([hi, lo], 0), normed_t[...], preferred_element_type=F32)
    router = (both[:experts] + both[experts:]).astype(BF16)
    for b in range(-(-width // 128)):
        lanes = min(128, width - b * 128)
        part[b, :, pl.ds(0, lanes)] = router[:, b * 128 : b * 128 + lanes]

    def scatter(order):
        for at in order:
            to = at // 2 * (n // 2) // half * 2 + at % 2
            b = at % 2 * half + at // 2

            @pl.when(to != me)
            def _(to=to, b=b):
                remote(part.at[b], rsbuf.at[me], rs_send.at[0], rs_recv.at[0], to // n_dp, to % n_dp).start()

    @pl.when(z < lines // 2)
    def _():
        scatter(range(owned - 1, -1, -1))

    @pl.when(z >= lines // 2)
    def _():
        scatter(range(owned))

    @pl.when(owner)
    def _():
        rsbuf[me] = part[mine]

    lax.fori_loop(cut1, cut2, wg_block, 0)

    @pl.when(owner)
    def _():
        all_of(rsbuf.at[pl.ds(0, n - 1)], rs_send.at[0], rs_recv.at[0]).wait_recv()
        agbuf[mine] = jnp.sum(rsbuf[...].astype(F32), 0).astype(BF16)

        def spread(k, _):
            i = jnp.where(z < lines // 2, n // 2 - 1 - k, k) * 2 + core

            @pl.when(i != me)
            def _():
                remote(
                    agbuf.at[mine], agbuf.at[mine], ag_send.at[0], ag_recv.at[0], i // n_dp, i % n_dp
                ).start()
            return 0

        lax.fori_loop(0, n // 2, spread, 0)

    rwt = rwt_s[...]
    ngrad = lax.dot_general(
        jnp.concatenate([rwt, rwt], 0), jnp.concatenate([hi, lo], 0), (((0,), (0,)), ((), ())),
        preferred_element_type=F32,
    )
    upper = ngrad * jnp.broadcast_to(gain_s[...].reshape(1, width), (tokens, width)).T
    unit = res_s[...].astype(F32) * inv_s[...]
    mean = jnp.mean(upper * unit, 0, keepdims=True)
    rg_ref[...] = (inv_s[...] * (upper - unit * mean)).astype(BF16)

    lax.fori_loop(cut2, blocks, wg_block, 0)

    for j in range(pieces):
        all_of(send[j].at[pl.ds(0, lines * (plane - 1))], row_send.at[j], row_recv.at[0, j]).wait_send()

    def finish_toks(source, _):
        def sent(side):
            nxt = z + 2 * side - 1

            @pl.when((nxt >= 0) & (nxt < lines))
            def _():
                all_of(tok.at[source], tok_send.at[source, side], tok_recv.at[source, 0]).wait_send()
                meta_copy(source, side).wait_send()

        @pl.when(source <= z)
        def _():
            sent(1)

        @pl.when(source >= z)
        def _():
            sent(0)
        return 0

    lax.fori_loop(0, lines, finish_toks, 0)
    all_of(ssend.at[pl.ds(0, n - 1)], sc_send.at[0], sc_recv.at[0]).wait_send()

    @pl.when(owner)
    def _():
        all_of(part.at[pl.ds(0, owned - 1)], rs_send.at[0], rs_recv.at[0]).wait_send()
        all_of(agbuf.at[pl.ds(0, half - 1)], ag_send.at[0], ag_recv.at[0]).wait_recv()

    @pl.when(jnp.logical_not(owner))
    def _():
        all_of(part, rs_send.at[0], rs_recv.at[0]).wait_send()
        all_of(agbuf.at[pl.ds(0, half)], ag_send.at[0], ag_recv.at[0]).wait_recv()

    to = me + 1 - 2 * core
    ours = agbuf.at[pl.ds(core * half, half)]
    twin = remote(ours, ours, twin_send.at[0], twin_recv.at[0], to // n_dp, to % n_dp)
    twin.start()
    twin.wait_recv()

    gain_row = gain_s[...].reshape(1, width)
    for b in range(-(-width // 128)):
        lanes = min(128, width - b * 128)
        at = slice(b * 128, b * 128 + lanes)
        total = agbuf[b, :, pl.ds(0, lanes)].astype(F32)
        rgt_ref[:, at] = total
        gg_ref[:, at] = jnp.sum(total * rwt_s[:, at].astype(F32), 0, keepdims=True) / gain_row[:, at]


    @pl.when(owner)
    def _():
        all_of(rsbuf.at[pl.ds(0, n // 2 - 1)], ag_send.at[0], ag_recv.at[0]).wait_send()

    twin.wait_send()


def store(hgt, wg, rg, rgt, gg, hgt_any, wg_any, rg_any, rgt_any, gg_any, sem):
    ff = wg.shape[0]
    blocks = max(b for b in range(1, 7) if ff % (b * 16) == 0)
    rows = ff // blocks
    copies = [
        pltpu.make_async_copy(wg.at[pl.ds(b * rows, rows)], wg_any.at[pl.ds(b * rows, rows)], sem.at[4 + b])
        for b in range(blocks)
    ]
    copies += [
        pltpu.make_async_copy(hgt, hgt_any, sem.at[0]),
        pltpu.make_async_copy(rg, rg_any, sem.at[1]),
        pltpu.make_async_copy(rgt, rgt_any, sem.at[2]),
        pltpu.make_async_copy(gg.at[0], gg_any, sem.at[3]),
    ]
    for c in copies:
        c.start()
    for c in copies:
        c.wait()


def column_cuts(width, pad_width):
    tiles = pad_width // 128
    ends = [tiles * sum(SHARES[: i + 1]) // sum(SHARES) for i in range(PIECES)]
    sizes = [e - b for b, e in zip([0] + ends, ends)]
    last = (tiles - sizes[0]) * 128
    cuts = [(last, width - last)]
    at = 0
    for s in sizes[1:]:
        cuts.append((at, s * 128))
        at += s * 128
    return tuple(cuts)


def on_device(n_ep, n_dp, residual, norm_gain, router_weight, out_grad, expert_ids, hidden, down_weight):
    n = n_ep * n_dp
    lines = math.gcd(n_ep, LINE)
    tokens, width = residual.shape
    topk = expert_ids.shape[1]
    experts = router_weight.shape[1]
    slots, ff = hidden.shape[1:]
    real_cap = slots // experts
    cap = -(-real_cap // 8) * 8
    pad_width = -(-(width + 1) // 128) * 128
    hidt = hidden[0].T
    if cap != real_cap:
        hidt = jnp.pad(
            hidt.reshape(ff, experts, real_cap), ((0, 0), (0, 0), (0, cap - real_cap))
        ).reshape(ff, experts * cap)
    rows = experts * cap
    plane = n // lines
    group = plane * cap
    owned = -(-width // 256) * 2
    assert owned <= n
    cuts = column_cuts(width, pad_width)
    rows_of_piece = [
        pltpu.VMEM((n, cap, lanes + (pad_width - width if j == 0 else 0)), BF16) for j, (_, lanes) in enumerate(cuts)
    ]
    vmem = pl.BlockSpec(memory_space=pltpu.VMEM)
    anyspace = pl.BlockSpec(memory_space=pl.ANY)
    dma = pltpu.SemaphoreType.DMA

    def far(x):
        return pltpu.with_memory_space_constraint(x, pltpu.HBM)

    outs = (((ff, rows), BF16), ((ff, width), BF16), ((width, tokens), BF16), ((experts, width), F32))
    held = pl.pallas_call(
        functools.partial(kernel, n_ep, n_dp, lines, cap, cuts),
        out_shape=tuple(pltpu.VMEM(s, t) for s, t in outs) + (pltpu.VMEM((1, width), F32),),
        in_specs=[anyspace] * 7,
        out_specs=(vmem,) * 5,
        scratch_shapes=[
            pltpu.VMEM((width, tokens), BF16),
            pltpu.VMEM((width,), F32),
            pltpu.VMEM((experts, width), BF16),
            pltpu.VMEM((topk, tokens), jnp.int32),
            pltpu.VMEM((lines, width, tokens), BF16),
            pltpu.VMEM((lines, -(-3 * topk // 16) * 16, tokens), BF16),
            pltpu.VMEM((2, group, tokens), BF16),
            rows_of_piece,
            rows_of_piece,
            pltpu.VMEM((ff, width), BF16),
            pltpu.VMEM((lines, ff, group), BF16),
            pltpu.VMEM((ff, rows), BF16),
            pltpu.VMEM((2, ff, group), F32),
            pltpu.VMEM((rows, width), BF16),
            pltpu.VMEM((tokens, width), BF16),
            pltpu.VMEM((1, tokens), F32),
            pltpu.VMEM((experts, tokens), F32),
            pltpu.VMEM((experts, tokens), F32),
            pltpu.VMEM((n, 1, 128), F32),
            pltpu.VMEM((n, 1, 128), F32),
            pltpu.VMEM((owned, experts, 128), BF16),
            pltpu.VMEM((n, experts, 128), BF16),
            pltpu.VMEM((owned, experts, 128), BF16),
            dma((7,)),
            dma((lines, 2)), dma((lines, PIECES)), dma((lines, 2)), dma((lines,)),
            dma((PIECES,)), dma((lines, PIECES)), dma((1,)), dma((1,)),
            dma((1,)), dma((1,)), dma((1,)), dma((1,)), dma((1,)), dma((1,)),
        ],
        compiler_params=pltpu.CompilerParams(
            collective_id=0, has_side_effects=True, vmem_limit_bytes=53_000_000
        ),
        name="expert_backward",
    )(*(far(x) for x in (residual.T, norm_gain, router_weight.T, out_grad.T, expert_ids.T, hidt, down_weight[0])))
    hgt, wg, rg, rgt, gg = pl.pallas_call(
        store,
        out_shape=tuple(jax.ShapeDtypeStruct(s, t) for s, t in outs) + (jax.ShapeDtypeStruct((width,), F32),),
        in_specs=[vmem] * 5,
        out_specs=(anyspace,) * 5,
        scratch_shapes=[dma((10,))],
        compiler_params=pltpu.CompilerParams(vmem_limit_bytes=2_000_000),
        name="store",
    )(*held)
    if cap != real_cap:
        hgt = hgt.reshape(ff, experts, cap)[:, :, :real_cap].reshape(ff, slots)
    return hgt.T[None], wg[None], rg.T, rgt.T, gg


def solution(mesh):
    both = ("ep", "dp")
    return jax.shard_map(
        functools.partial(on_device, mesh.shape["ep"], mesh.shape["dp"]),
        mesh=mesh,
        in_specs=(P(both, None), P(), P(), P(both, None), P(both, None), P(both, None, None), P(both, None, None)),
        out_specs=(P(both, None, None), P(both, None, None), P(both, None), P(), P()),
        check_vma=False,
    )
```

```python
import functools
import math

import jax
import jax.numpy as jnp
from jax import lax
from jax.experimental import pallas as pl
from jax.experimental.pallas import tpu as pltpu
from jax.sharding import PartitionSpec as P

F32 = jnp.float32
BF16 = jnp.bfloat16
LINE = 4
SHARES = (9, 7, 4, 3)
PIECES = len(SHARES)
LAG = 2


def kernel(
    n_ep, n_dp, lines, cap, cuts,
    res_any, gain_any, rwt_any, og_any, ids_any, hidt_any, w_any,
    hgt, wg, rg_ref, rgt_ref, gg_ref,
    res_s, gain_s, rwt_s, ids_s, tok, meta, hot_s, send, recv, w, hid3, hidt, inner_s, scaled, normed_t, inv_s,
    prob_s, rank_s, ssend, srecv, part, rsbuf, agbuf,
    in_sem, tok_send, tok_recv, meta_send, meta_recv, row_send, row_recv, sc_send, sc_recv, rs_send, rs_recv, ag_send, ag_recv, twin_send, twin_recv,
):
    n = n_ep * n_dp
    width, tokens = res_s.shape
    experts = rwt_s.shape[0]
    ff = w.shape[0]
    spare = send[0].shape[2] - cuts[0][1]
    plane = n // lines
    group = plane * cap
    pieces = len(cuts)
    owned = part.shape[0]
    me = lax.axis_index("ep") * n_dp + lax.axis_index("dp")
    half = owned // 2
    core = me % 2
    seat = (me // 2 * half + n // 2 - 1) // (n // 2)
    owner = seat * (n // 2) < (me // 2 + 1) * half
    mine = core * half + seat
    z = me // plane
    p = me % plane

    def remote(src, dst, s_sem, r_sem, dev_ep, dev_dp):
        return pltpu.make_async_remote_copy(
            src_ref=src, dst_ref=dst, send_sem=s_sem, recv_sem=r_sem,
            device_id=(dev_ep, dev_dp), device_id_type=pl.DeviceIdType.MESH,
        )

    barrier = pltpu.get_barrier_semaphore()

    def hello(to):
        pl.semaphore_signal(
            barrier, inc=1, device_id=(to // n_dp, to % n_dp), device_id_type=pl.DeviceIdType.MESH
        )

    for side in range(2):
        nxt = z + 2 * side - 1

        @pl.when((nxt >= 0) & (nxt < lines))
        def _():
            hello(nxt * plane + p)

    def greet(k, _):
        hello(z * plane + (p + k) % plane)
        return 0

    lax.fori_loop(1, plane, greet, 0)

    load_og = pltpu.make_async_copy(og_any, tok.at[z], in_sem.at[0])
    loads = [
        pltpu.make_async_copy(res_any, res_s, in_sem.at[1]),
        pltpu.make_async_copy(gain_any, gain_s, in_sem.at[2]),
        pltpu.make_async_copy(rwt_any, rwt_s, in_sem.at[3]),
        pltpu.make_async_copy(ids_any, ids_s, in_sem.at[4]),
    ]
    load_h = pltpu.make_async_copy(hidt_any, hidt, in_sem.at[5])
    load_w = pltpu.make_async_copy(w_any, w, in_sem.at[6])
    load_og.start()
    for c in loads:
        c.start()
    load_h.start()
    load_w.start()

    def tok_copy(source, side, j):
        to = (z + 2 * side - 1) * plane + p
        at = pl.ds(cuts[j][0], cuts[j][1])
        return remote(
            tok.at[source, at], tok.at[source, at], tok_send.at[source, side], tok_recv.at[source, j],
            to // n_dp, to % n_dp,
        )

    def meta_copy(source, side):
        to = (z + 2 * side - 1) * plane + p
        return remote(
            meta.at[source], meta.at[source], meta_send.at[source, side], meta_recv.at[source],
            to // n_dp, to % n_dp,
        )

    def along(source, side, j):
        return [tok_copy(source, side, j)] + ([meta_copy(source, side)] if j == 0 else [])

    def to_side(side, copies):
        nxt = z + 2 * side - 1

        @pl.when((nxt >= 0) & (nxt < lines))
        def _():
            for c in copies:
                c.start()

    ssend[...] = jnp.zeros_like(ssend)
    for b in range(width // 128, owned):
        part[b] = jnp.zeros(part.shape[1:], BF16)
    load_og.wait()
    neighbours = jnp.where(z > 0, 1, 0) + jnp.where(z < lines - 1, 1, 0)
    pl.semaphore_wait(barrier, plane - 1 + neighbours)
    for side in range(2):
        to_side(side, [tok_copy(z, side, 0)])

    for c in loads:
        c.wait()
    gain_row = gain_s[...].reshape(1, width)
    gain = jnp.broadcast_to(gain_row, (tokens, width)).T
    floated = res_s[...].astype(F32)
    inverse = lax.rsqrt(jnp.mean(floated * floated, 0, keepdims=True) + 1e-05)
    unit = floated * inverse
    normed = (unit * gain).astype(BF16)
    inv_s[...] = inverse
    normed_t[...] = normed.T
    logits = jnp.dot(rwt_s[...], normed, preferred_element_type=F32)
    row_e = lax.broadcasted_iota(jnp.int32, (experts, tokens), 0)
    match = jnp.zeros((experts, tokens), F32)
    ids = ids_s[...]
    for k in range(ids.shape[0]):
        match = match + jnp.where(ids[k : k + 1, :] == row_e, F32(1.0), F32(0.0))
    expo = jnp.where(match > 0, jnp.exp(logits), F32(0.0))
    prob = expo / jnp.sum(expo, 0, keepdims=True)
    row_t = lax.broadcasted_iota(jnp.int32, (tokens, tokens), 0)
    col_t = lax.broadcasted_iota(jnp.int32, (tokens, tokens), 1)
    before = jnp.where(row_t < col_t, F32(1.0), F32(0.0)).astype(BF16)
    rank = jnp.dot(match.astype(BF16), before, preferred_element_type=F32)
    rank = jnp.where(match > 0, rank, F32(-1.0))
    prob_s[...] = prob
    rank_s[...] = rank
    topk = ids.shape[0]

    def chosen(values):
        return [
            jnp.sum(jnp.where(ids[k : k + 1, :] == row_e, values, F32(0.0)), 0, keepdims=True) for k in range(topk)
        ]

    unused = meta.shape[1] - 3 * topk
    info = [ids.astype(F32)] + chosen(rank) + chosen(prob)
    if unused:
        info.append(jnp.zeros((unused, tokens), F32))
    meta[z] = jnp.concatenate(info, 0).astype(BF16)

    for side in range(2):
        to_side(side, [meta_copy(z, side)])
    for j in range(1, pieces):
        for side in range(2):
            to_side(side, [tok_copy(z, side, j)])

    def sides(k, fn):
        def step(i, _):
            source = z + k * (2 * i - 1)

            @pl.when((source >= 0) & (source < lines) & (k + 1 - i > 0) & (k >= 0))
            def _():
                fn(source, i)
            return 0
        lax.fori_loop(0, 2, step, 0)

    def onward(i):
        nxt = z + 1 - 2 * i
        return (nxt >= 0) & (nxt < lines)

    def relay(j, source, i):
        @pl.when(onward(i))
        def _():
            for c in along(source, i, j):
                c.wait_recv()
            for c in along(source, 1 - i, j):
                c.start()

    def settle(j, source, i):
        @pl.when(jnp.logical_not(onward(i)))
        def _():
            for c in along(source, i, j):
                c.wait_recv()

    def pack(j, source, i):
        first = source * plane
        lane0, lanes = cuts[j]
        if j == 0:
            info = meta[source].astype(F32)
            expert = (lax.broadcasted_iota(jnp.int32, (plane, 1, tokens), 0) + z * plane).astype(F32)
            rt = jnp.full((plane, 1, tokens), -1.0, F32)
            pt = jnp.zeros((plane, 1, tokens), F32)
            for k in range(topk):
                here = expert == info[k : k + 1].reshape(1, 1, tokens)
                rt = jnp.where(here, info[topk + k : topk + k + 1].reshape(1, 1, tokens), rt)
                pt = jnp.where(here, info[2 * topk + k : 2 * topk + k + 1].reshape(1, 1, tokens), pt)
            slot = lax.broadcasted_iota(jnp.int32, (plane, cap, tokens), 1).astype(F32)
            hit = slot == rt
            hot = jnp.where(hit, F32(1.0), F32(0.0)).reshape(group, tokens).astype(BF16)
            weight = jnp.sum(jnp.where(hit, pt, F32(0.0)), -1, keepdims=True)
            hot_s[i] = hot
            send[0][pl.ds(first, plane), :, pl.ds(lanes, spare)] = jnp.broadcast_to(
                weight, (plane, cap, spare)
            ).astype(BF16)
        else:
            hot = hot_s[i]
        rows = lax.dot_general(
            hot, tok[source, pl.ds(lane0, lanes)], (((1,), (1,)), ((), ())), preferred_element_type=F32
        )
        send[j][pl.ds(first, plane), :, pl.ds(0, lanes)] = rows.reshape(plane, cap, lanes).astype(BF16)
        own = first + p
        recv[j][own] = send[j][own]

        if plane > 8:
            def push(k, _):
                row_copy(source, partner(plane - k), p, j).start()
                return 0

            lax.fori_loop(1, plane, push, 0)
        else:
            for k in range(1, plane):
                row_copy(source, partner(plane - k), p, j).start()

    def partner(k):
        if plane & (plane - 1):
            return (p + k) % plane
        bits = range(plane.bit_length() - 1)
        return sum((p // (1 << b) + k // (1 << b)) % 2 * (1 << b) for b in bits)

    def row_copy(source, q, slot, j):
        first = source * plane
        to = z * plane + q
        return remote(
            send[j].at[first + q], recv[j].at[first + slot], row_send.at[j], row_recv.at[source, j],
            to // n_dp, to % n_dp,
        )

    def all_of(ref, s_sem, r_sem):
        return remote(ref, ref, s_sem, r_sem, 0, 0)

    def chunk(j, source, i):
        first = source * plane
        lane0, lanes = cuts[j]

        landed = recv[j].at[pl.ds(first, plane - 1)]
        all_of(landed, row_send.at[j], row_recv.at[source, j]).wait_recv()
        at = pl.ds(pl.multiple_of(first * cap, group), group)
        tail = recv[0][pl.ds(first, plane), :, pl.ds(cuts[0][1] + spare - 128, 128)].astype(F32).reshape(group, 128)
        weight = tail[:, 128 - spare : 129 - spare]
        grad = recv[j][pl.ds(first, plane), :, pl.ds(0, lanes)].astype(F32).reshape(group, lanes)
        inner = lax.dot_general(
            w[:, lane0 : lane0 + lanes], grad.astype(BF16), (((1,), (1,)), ((), ())), preferred_element_type=F32
        )
        if j > 0:
            inner = inner_s[i] + inner
        if j < pieces - 1:
            inner_s[i] = inner
        else:
            score = jnp.sum(inner * hid3[source].astype(F32), 0, keepdims=True)
            for k in range(plane):
                ssend[first + k, :, pl.ds(0, cap)] = score[:, k * cap : (k + 1) * cap]

            def push(k, _):
                d = first + k

                @pl.when(d != me)
                def _():
                    remote(
                        ssend.at[d], srecv.at[me], sc_send.at[0], sc_recv.at[0], d // n_dp, d % n_dp
                    ).start()
                return 0

            lax.fori_loop(0, plane, push, 0)

            @pl.when(source == z)
            def _():
                srecv[me] = ssend[me]

            across = jnp.broadcast_to(weight, (group, 128)).T[0:1, :]
            grad_h = (across * inner).astype(BF16)
            for b in range(lines):
                @pl.when(source == b)
                def _(b=b):
                    hgt[:, b * group : (b + 1) * group] = grad_h
        scaled[at, lane0 : lane0 + lanes] = (weight * grad).astype(BF16)

    def stage(k, _):
        for j in range(pieces):
            @pl.when((k > 0) & (k < lines))
            def _(j=j):
                sides(k, functools.partial(settle, j))

            @pl.when(k < lines)
            def _(j=j):
                sides(k, functools.partial(pack, j))

            later = k + (j + 1) // pieces

            @pl.when((later > 0) & (later < lines))
            def _(j=j, later=later):
                sides(later, functools.partial(relay, (j + 1) % pieces))

            if j == min(LAG, pieces - 1):
                @pl.when(k == 0)
                def _():
                    load_h.wait()
                    for i in range(lines):
                        hid3[i] = hidt[:, i * group : (i + 1) * group]
                    load_w.wait()

            sides(k + (j - LAG) // pieces, functools.partial(chunk, (j - LAG) % pieces))
        return 0

    lax.fori_loop(0, lines + 1, stage, 0)

    blocks = max(b for b in range(1, 6) if ff % (b * 16) == 0)
    rows_of = ff // blocks

    def wg_block(b, _):
        at = pl.ds(pl.multiple_of(b * rows_of, rows_of), rows_of)
        wg[at] = jnp.dot(hidt[at], scaled[...], preferred_element_type=F32).astype(BF16)
        return 0

    cut1, cut2 = (2 * blocks) // 5, (4 * blocks) // 5
    lax.fori_loop(0, cut1, wg_block, 0)

    all_of(srecv.at[pl.ds(0, n - 1)], sc_send.at[0], sc_recv.at[0]).wait_recv()
    back = srecv[...].reshape(n, 128)
    rank = rank_s[...]
    prob = prob_s[...]
    score = jnp.zeros((experts, tokens), F32)
    for r in range(cap):
        score = score + jnp.where(rank == F32(r), back[:, r : r + 1], F32(0.0))
    lg = prob * (score - jnp.sum(prob * score, 0, keepdims=True))
    hi = lg.astype(BF16)
    lo = (lg - hi.astype(F32)).astype(BF16)
    stacked = jnp.concatenate([hi, lo], 0)

    def scatter(order):
        for at in order:
            to = at // 2 * (n // 2) // half * 2 + at % 2
            b = at % 2 * half + at // 2

            @pl.when(to != me)
            def _(to=to, b=b):
                remote(part.at[b], rsbuf.at[me], rs_send.at[0], rs_recv.at[0], to // n_dp, to % n_dp).start()

    for side in range(2):
        first = side * half * 128
        lanes = min(width - first, half * 128)
        both = jnp.dot(stacked, normed_t[:, first : first + lanes], preferred_element_type=F32)
        router = (both[:experts] + both[experts:]).astype(BF16)
        for t in range(-(-lanes // 128)):
            end = min(t * 128 + 128, lanes)
            part[side * half + t, :, pl.ds(0, end - t * 128)] = router[:, t * 128 : end]

        @pl.when(z < lines // 2)
        def _(side=side):
            scatter(range(owned - 2 + side, -1, -2))

        @pl.when(z >= lines // 2)
        def _(side=side):
            scatter(range(side, owned, 2))

    @pl.when(owner)
    def _():
        rsbuf[me] = part[mine]

    lax.fori_loop(cut1, cut2, wg_block, 0)

    @pl.when(owner)
    def _():
        all_of(rsbuf.at[pl.ds(0, n - 1)], rs_send.at[0], rs_recv.at[0]).wait_recv()
        agbuf[mine] = jnp.sum(rsbuf[...].astype(F32), 0).astype(BF16)

        def spread(k, _):
            i = jnp.where(z < lines // 2, n // 2 - 1 - k, k) * 2 + core

            @pl.when(i != me)
            def _():
                remote(
                    agbuf.at[mine], agbuf.at[mine], ag_send.at[0], ag_recv.at[0], i // n_dp, i % n_dp
                ).start()
            return 0

        lax.fori_loop(0, n // 2, spread, 0)

    rwt = rwt_s[...]
    ngrad = lax.dot_general(
        jnp.concatenate([rwt, rwt], 0), jnp.concatenate([hi, lo], 0), (((0,), (0,)), ((), ())),
        preferred_element_type=F32,
    )
    upper = ngrad * jnp.broadcast_to(gain_s[...].reshape(1, width), (tokens, width)).T
    unit = res_s[...].astype(F32) * inv_s[...]
    mean = jnp.mean(upper * unit, 0, keepdims=True)
    rg_ref[...] = (inv_s[...] * (upper - unit * mean)).astype(BF16)

    lax.fori_loop(cut2, blocks, wg_block, 0)

    for j in range(pieces):
        all_of(send[j].at[pl.ds(0, lines * (plane - 1))], row_send.at[j], row_recv.at[0, j]).wait_send()

    def finish_toks(source, _):
        def sent(side):
            nxt = z + 2 * side - 1

            @pl.when((nxt >= 0) & (nxt < lines))
            def _():
                all_of(tok.at[source], tok_send.at[source, side], tok_recv.at[source, 0]).wait_send()
                meta_copy(source, side).wait_send()

        @pl.when(source <= z)
        def _():
            sent(1)

        @pl.when(source >= z)
        def _():
            sent(0)
        return 0

    lax.fori_loop(0, lines, finish_toks, 0)
    all_of(ssend.at[pl.ds(0, n - 1)], sc_send.at[0], sc_recv.at[0]).wait_send()

    @pl.when(owner)
    def _():
        all_of(part.at[pl.ds(0, owned - 1)], rs_send.at[0], rs_recv.at[0]).wait_send()
        all_of(agbuf.at[pl.ds(0, half - 1)], ag_send.at[0], ag_recv.at[0]).wait_recv()

    @pl.when(jnp.logical_not(owner))
    def _():
        all_of(part, rs_send.at[0], rs_recv.at[0]).wait_send()
        all_of(agbuf.at[pl.ds(0, half)], ag_send.at[0], ag_recv.at[0]).wait_recv()

    to = me + 1 - 2 * core
    ours = agbuf.at[pl.ds(core * half, half)]
    twin = remote(ours, ours, twin_send.at[0], twin_recv.at[0], to // n_dp, to % n_dp)
    twin.start()
    twin.wait_recv()

    gain_row = gain_s[...].reshape(1, width)
    for b in range(-(-width // 128)):
        lanes = min(128, width - b * 128)
        at = slice(b * 128, b * 128 + lanes)
        total = agbuf[b, :, pl.ds(0, lanes)].astype(F32)
        rgt_ref[:, at] = total
        gg_ref[:, at] = jnp.sum(total * rwt_s[:, at].astype(F32), 0, keepdims=True) / gain_row[:, at]


    @pl.when(owner)
    def _():
        all_of(rsbuf.at[pl.ds(0, n // 2 - 1)], ag_send.at[0], ag_recv.at[0]).wait_send()

    twin.wait_send()


def store(hgt, wg, rg, rgt, gg, hgt_any, wg_any, rg_any, rgt_any, gg_any, sem):
    ff = wg.shape[0]
    blocks = max(b for b in range(1, 7) if ff % (b * 16) == 0)
    rows = ff // blocks
    copies = [
        pltpu.make_async_copy(wg.at[pl.ds(b * rows, rows)], wg_any.at[pl.ds(b * rows, rows)], sem.at[4 + b])
        for b in range(blocks)
    ]
    copies += [
        pltpu.make_async_copy(hgt, hgt_any, sem.at[0]),
        pltpu.make_async_copy(rg, rg_any, sem.at[1]),
        pltpu.make_async_copy(rgt, rgt_any, sem.at[2]),
        pltpu.make_async_copy(gg.at[0], gg_any, sem.at[3]),
    ]
    for c in copies:
        c.start()
    for c in copies:
        c.wait()


def column_cuts(width, pad_width):
    tiles = pad_width // 128
    ends = [tiles * sum(SHARES[: i + 1]) // sum(SHARES) for i in range(PIECES)]
    sizes = [e - b for b, e in zip([0] + ends, ends)]
    last = (tiles - sizes[0]) * 128
    cuts = [(last, width - last)]
    at = 0
    for s in sizes[1:]:
        cuts.append((at, s * 128))
        at += s * 128
    return tuple(cuts)


def on_device(n_ep, n_dp, residual, norm_gain, router_weight, out_grad, expert_ids, hidden, down_weight):
    n = n_ep * n_dp
    lines = math.gcd(n_ep, LINE)
    tokens, width = residual.shape
    topk = expert_ids.shape[1]
    experts = router_weight.shape[1]
    slots, ff = hidden.shape[1:]
    real_cap = slots // experts
    cap = -(-real_cap // 8) * 8
    pad_width = -(-(width + 1) // 128) * 128
    hidt = hidden[0].T
    if cap != real_cap:
        hidt = jnp.pad(
            hidt.reshape(ff, experts, real_cap), ((0, 0), (0, 0), (0, cap - real_cap))
        ).reshape(ff, experts * cap)
    rows = experts * cap
    plane = n // lines
    group = plane * cap
    owned = -(-width // 256) * 2
    assert owned <= n
    cuts = column_cuts(width, pad_width)
    rows_of_piece = [
        pltpu.VMEM((n, cap, lanes + (pad_width - width if j == 0 else 0)), BF16) for j, (_, lanes) in enumerate(cuts)
    ]
    vmem = pl.BlockSpec(memory_space=pltpu.VMEM)
    anyspace = pl.BlockSpec(memory_space=pl.ANY)
    dma = pltpu.SemaphoreType.DMA

    def far(x):
        return pltpu.with_memory_space_constraint(x, pltpu.HBM)

    outs = (((ff, rows), BF16), ((ff, width), BF16), ((width, tokens), BF16), ((experts, width), F32))
    held = pl.pallas_call(
        functools.partial(kernel, n_ep, n_dp, lines, cap, cuts),
        out_shape=tuple(pltpu.VMEM(s, t) for s, t in outs) + (pltpu.VMEM((1, width), F32),),
        in_specs=[anyspace] * 7,
        out_specs=(vmem,) * 5,
        scratch_shapes=[
            pltpu.VMEM((width, tokens), BF16),
            pltpu.VMEM((width,), F32),
            pltpu.VMEM((experts, width), BF16),
            pltpu.VMEM((topk, tokens), jnp.int32),
            pltpu.VMEM((lines, width, tokens), BF16),
            pltpu.VMEM((lines, -(-3 * topk // 16) * 16, tokens), BF16),
            pltpu.VMEM((2, group, tokens), BF16),
            rows_of_piece,
            rows_of_piece,
            pltpu.VMEM((ff, width), BF16),
            pltpu.VMEM((lines, ff, group), BF16),
            pltpu.VMEM((ff, rows), BF16),
            pltpu.VMEM((2, ff, group), F32),
            pltpu.VMEM((rows, width), BF16),
            pltpu.VMEM((tokens, width), BF16),
            pltpu.VMEM((1, tokens), F32),
            pltpu.VMEM((experts, tokens), F32),
            pltpu.VMEM((experts, tokens), F32),
            pltpu.VMEM((n, 1, 128), F32),
            pltpu.VMEM((n, 1, 128), F32),
            pltpu.VMEM((owned, experts, 128), BF16),
            pltpu.VMEM((n, experts, 128), BF16),
            pltpu.VMEM((owned, experts, 128), BF16),
            dma((7,)),
            dma((lines, 2)), dma((lines, PIECES)), dma((lines, 2)), dma((lines,)),
            dma((PIECES,)), dma((lines, PIECES)), dma((1,)), dma((1,)),
            dma((1,)), dma((1,)), dma((1,)), dma((1,)), dma((1,)), dma((1,)),
        ],
        compiler_params=pltpu.CompilerParams(
            collective_id=0, has_side_effects=True, vmem_limit_bytes=53_000_000
        ),
        name="expert_backward",
    )(*(far(x) for x in (residual.T, norm_gain, router_weight.T, out_grad.T, expert_ids.T, hidt, down_weight[0])))
    hgt, wg, rg, rgt, gg = pl.pallas_call(
        store,
        out_shape=tuple(jax.ShapeDtypeStruct(s, t) for s, t in outs) + (jax.ShapeDtypeStruct((width,), F32),),
        in_specs=[vmem] * 5,
        out_specs=(anyspace,) * 5,
        scratch_shapes=[dma((10,))],
        compiler_params=pltpu.CompilerParams(vmem_limit_bytes=2_000_000),
        name="store",
    )(*held)
    if cap != real_cap:
        hgt = hgt.reshape(ff, experts, cap)[:, :, :real_cap].reshape(ff, slots)
    return hgt.T[None], wg[None], rg.T, rgt.T, gg


def solution(mesh):
    both = ("ep", "dp")
    return jax.shard_map(
        functools.partial(on_device, mesh.shape["ep"], mesh.shape["dp"]),
        mesh=mesh,
        in_specs=(P(both, None), P(), P(), P(both, None), P(both, None), P(both, None, None), P(both, None, None)),
        out_specs=(P(both, None, None), P(both, None, None), P(both, None), P(), P()),
        check_vma=False,
    )
```
